32 devices in a mesh: gx: 8 (over z, x), gy: 4 (over y, core).
Axes of the slice: x: 2, y: 2, z: 4, core: 2. Of those that a mesh axis runs over, the one named last changes fastest.
Arguments:
- rhs: float32 [128, 128, 128], P('gx', 'gy'), may hold values from -6 to 6
- target: float32 [128, 128, 128], P('gx', 'gy'), may hold values from -6 to 6
- stencils: float32 [9, 27], replicated, may hold values from -0.006 to 0.11, as said below
- face_mask: int32 [6], replicated, may hold values 0 or 1
Outputs:
- solution: float32 [128, 128, 128], P('gx', 'gy')
- grad_rhs: float32 [128, 128, 128], P('gx', 'gy')
- grad_stencils: float32 [9, 27], replicated
The draws below stay inside these ranges and needn't reach their ends.
Inputs may be any that keep to these rules, and one draw needn't show every extreme that they name: `stencils`: entry 13 of every row lies in 0.05 to 0.11, entries 4, 10, 12, 14, 16, 22 in 0.005 to 0.02, the others in -0.006 to 0.006.
All inputs are finite; a program needn't handle non-finite values.
Results may differ from the reference program's by a relative error of at most 0.00002.
Values sent between devices are 32-bit elements; how exact they have to be, the bound alone decides.
No kernel may reach another device: no remote copies, remote signals or barrier semaphores. Data moves between devices by JAX's collectives and lax.ppermute only.
A program may use at most 128 MiB of HBM per device.

```python
import jax
import jax.numpy as jnp

NZ = 128
LEVELS = 4
SWEEPS = 3
NX = 128
NY = 128
CELLS = 2097152


def draw_stencils(key, part):
    rows = 2 * LEVELS + 1
    key_center, key_face, key_other = jax.random.split(jax.random.fold_in(key, 17), 3)
    center = jax.random.uniform(key_center, (rows, 27), jnp.float32, 0.06, 0.1)
    facing = jax.random.uniform(key_face, (rows, 27), jnp.float32, 0.005, 0.02)
    others = jax.random.uniform(key_other, (rows, 27), jnp.float32, -0.006, 0.006)
    column = jnp.arange(27)
    is_face = (column == 4) | (column == 10) | (column == 12) | (column == 14) | (column == 16) | (column == 22)
    picked = jnp.where(column == 13, center, jnp.where(is_face, facing, others))
    return picked.astype(jnp.float32)


def touch_ends(values, rng, smallest, high):
    shape = values.shape
    place = [jax.random.randint(jax.random.fold_in(rng, axis), (), 0, shape[axis]) for axis in range(len(shape))]
    values = values.at[tuple(place)].set(smallest)
    longest = shape.index(max(shape))
    place[longest] = (place[longest] + 1) % shape[longest]
    return values.at[tuple(place)].set(high)


def block_levels(key, dims, shards, least, high):
    level, own = 1.0, jax.random.fold_in(key, 6)
    for dim, shards_of in shards:
        steps = jnp.exp(jax.random.uniform(jax.random.fold_in(own, dim), (shards_of,), jnp.float32, least / len(shards), high / len(shards)))
        level = level * jnp.repeat(steps, dims[dim] // shards_of).reshape([-1 if axis == dim else 1 for axis in range(len(dims))])
    return level


def bell_draw(rng, shape, deviation, reach, cuts=(), kind=jnp.bfloat16):
    entries = deviation * jax.random.normal(rng, shape, jnp.float32)
    if cuts:
        entries = entries * block_levels(rng, shape, cuts, -0.22, 0.18)
    return jnp.clip(entries, -reach, reach).astype(kind)


def setup_inputs(seed: int = 0) -> dict:
    arg_keys = jax.random.split(jax.random.key(seed), 5)
    rhs = bell_draw(arg_keys[0], (NX, NY, NZ), 1.0, 6.0, ((0, 8), (1, 4)), jnp.float32)
    target = bell_draw(arg_keys[1], (NX, NY, NZ), 1.0, 6.0, ((0, 8), (1, 4)), jnp.float32)
    stencils = draw_stencils(jax.random.fold_in(arg_keys[4], 71), 0)
    face_mask = touch_ends((jax.random.randint(arg_keys[3], (6,), 0, 2) < 1).astype(jnp.int32), jax.random.fold_in(arg_keys[3], 1), 0, 1)
    return dict(rhs=rhs, target=target, stencils=stencils, face_mask=face_mask)


def shifted_sum(padded, weights, shape):
    total = jnp.zeros(shape, jnp.float32)
    for shift_first in range(3):
        for shift_second in range(3):
            for shift_third in range(3):
                window = padded[shift_first:shift_first + shape[0], shift_second:shift_second + shape[1], shift_third:shift_third + shape[2]]
                total = total + weights[9 * shift_first + 3 * shift_second + shift_third] * window
    return total

def smooth(field, weights):
    return shifted_sum(jnp.pad(field, 1), weights, field.shape)

def face_tally(shape, face_mask):
    walls = face_mask.astype(jnp.float32)
    first = jnp.arange(shape[0])[:, None, None]
    second = jnp.arange(shape[1])[None, :, None]
    third = jnp.arange(shape[2])[None, None, :]
    tally = walls[0] * (first == 0).astype(jnp.float32) + walls[1] * (first == shape[0] - 1).astype(jnp.float32)
    tally = tally + walls[2] * (second == 0).astype(jnp.float32) + walls[3] * (second == shape[1] - 1).astype(jnp.float32)
    tally = tally + walls[4] * (third == 0).astype(jnp.float32) + walls[5] * (third == shape[2] - 1).astype(jnp.float32)
    return tally

def operate(field, tally):
    padded = jnp.pad(field, 1)
    beside = padded[2:, 1:-1, 1:-1] + padded[:-2, 1:-1, 1:-1]
    beside = beside + padded[1:-1, 2:, 1:-1] + padded[1:-1, :-2, 1:-1]
    beside = beside + padded[1:-1, 1:-1, 2:] + padded[1:-1, 1:-1, :-2]
    return (6.0 - tally) * field - beside

def restrict(field):
    shape = field.shape
    return field.reshape(shape[0] // 2, 2, shape[1] // 2, 2, shape[2]).mean(axis=(1, 3))

def prolong(field):
    return jnp.repeat(jnp.repeat(field, 2, axis=0), 2, axis=1)

def cycle(source, stencils, face_mask, height):
    tally = face_tally(source.shape, face_mask)
    if height == LEVELS:
        weights = stencils[2 * LEVELS]
        iterate = smooth(source, weights)
        for sweep_index in range(SWEEPS - 1):
            iterate = iterate + smooth(source - operate(iterate, tally), weights)
        return iterate
    presmooth = smooth(source, stencils[height])
    coarse = cycle(restrict(source - operate(presmooth, tally)), stencils, face_mask, height + 1)
    middle = presmooth + prolong(coarse)
    return middle + smooth(source - operate(middle, tally), stencils[LEVELS + height])

def reference(rhs, target, stencils, face_mask):
    solution, pullback = jax.vjp(lambda source, weights: cycle(source, weights, face_mask, 0), rhs, stencils)
    error = solution - target
    grad_rhs, grad_weights = pullback(error)
    return (solution, grad_rhs, grad_weights / CELLS)
```

```python
import functools

import jax
import jax.numpy as jnp
from jax import lax
from jax.experimental import pallas as pl
from jax.experimental.pallas import tpu as pltpu
from jax.sharding import PartitionSpec as P

LEVELS = 4
SWEEPS = 3
LOCAL = 2
RIM0 = 10
RIM1 = 4
KEEP = 2
ROWS, COLS = 2, 8
PEERS = ("gx", "gy")


def starts(width):
    places = list(range(0, width - 7, 8))
    if width % 8:
        places.append(width - 8)
    return places


def lanes(shape=(8, 128)):
    return lax.broadcasted_iota(jnp.int32, shape, 1)


def sublanes(shape=(8, 128)):
    return lax.broadcasted_iota(jnp.int32, shape, 0)


def from_below(value):
    return jnp.where(lanes(value.shape) == 0, 0.0, pltpu.roll(value, 1, 1))


def from_above(value):
    last = value.shape[1] - 1
    return jnp.where(lanes(value.shape) == last, 0.0, pltpu.roll(value, last, 1))


def weights_of(stencils, row, flip):
    return [stencils[row, 26 - t if flip else t] for t in range(27)]


class Level:
    def __init__(self, walls, first, second, total_first, total_second):
        self.walls = walls
        self.first = first
        self.second = second
        self.total = (total_first, total_second)

    def row_wall(self, row):
        at = self.first + row
        return jnp.where(at == 0, self.walls[0], 0.0) + jnp.where(
            at == self.total[0] - 1, self.walls[1], 0.0
        )

    def row_inside(self, row):
        at = self.first + row
        return (at >= 0) & (at < self.total[0])

    def wall_plane(self, col):
        at = self.second + col + sublanes()
        lane = lanes()
        plane = jnp.where(at == 0, self.walls[2], 0.0)
        plane = plane + jnp.where(at == self.total[1] - 1, self.walls[3], 0.0)
        plane = plane + jnp.where(lane == 0, self.walls[4], 0.0)
        return plane + jnp.where(lane == 127, self.walls[5], 0.0)

    def inside(self, row, col):
        at = self.second + col + sublanes()
        return self.row_inside(row) & (at >= 0) & (at < self.total[1])


def smoothed(source, weights, row, col):
    sums = [None, None, None]
    for a in range(3):
        for b in range(3):
            window = source[row + (a - 1), pl.ds(col + (b - 1), 8), :]
            for c in range(3):
                term = weights[9 * a + 3 * b + c] * window
                sums[c] = term if sums[c] is None else sums[c] + term
    return sums[1] + from_below(sums[0]) + from_above(sums[2])


def applied(source, level, row, col, at_row, at_col):
    here = source[row, pl.ds(col, 8), :]
    beside = source[row - 1, pl.ds(col, 8), :] + source[row + 1, pl.ds(col, 8), :]
    beside = beside + source[row, pl.ds(col - 1, 8), :] + source[row, pl.ds(col + 1, 8), :]
    beside = beside + from_below(here) + from_above(here)
    diagonal = (6.0 - level.row_wall(at_row)) - level.wall_plane(at_col)
    return diagonal * here - beside


def each(rows, cols, zero, body):
    places = starts(cols)

    def step(row, carry):
        for place in places:
            body(row, zero + place)
        return carry

    lax.fori_loop(0, rows, step, 0)


def smooth_into(out, source, weights, level, start, size, origin, zero, masked=True, add=None):
    def body(row, col):
        row, col = row + start[0], col + start[1]
        value = smoothed(source, weights, row, col)
        if masked:
            value = jnp.where(level.inside(row - origin[0], col - origin[1]), value, 0.0)
        if add is not None:
            value = value + add[row, pl.ds(col, 8), :]
        out[row, pl.ds(col, 8), :] = value

    each(size[0], size[1], zero, body)


def remain_into(out, right, source, level, start, size, origin, zero, masked=True):
    def body(row, col):
        row, col = row + start[0], col + start[1]
        value = right[row, pl.ds(col, 8), :] - applied(
            source, level, row, col, row - origin[0], col - origin[1]
        )
        if masked:
            value = jnp.where(level.inside(row - origin[0], col - origin[1]), value, 0.0)
        out[row, pl.ds(col, 8), :] = value

    each(size[0], size[1], zero, body)


def restrict_into(out, place, right, source, line, fine, coarse, start, size, origin, zero, masked):
    wide = starts(2 * size[1])
    narrow = starts(size[1])

    def step(row, carry):
        for col in wide:
            col = col + zero
            total = None
            for half in range(2):
                at_row, at_col = start[0] + 2 * row + half, start[1] + col
                value = right[at_row, pl.ds(at_col, 8), :] - applied(
                    source, fine, at_row, at_col, at_row - origin[0], at_col - origin[1]
                )
                total = value if total is None else total + value
            line[pl.ds(col, 8), :] = total
        for col in narrow:
            value = line[pl.ds(2 * col, 8, stride=2), :] + line[pl.ds(2 * col + 1, 8, stride=2), :]
            value = 0.25 * value
            if masked is not None:
                value = jnp.where(
                    coarse.inside(place[0] + row - masked[0], place[1] + col + zero - masked[1]),
                    value,
                    0.0,
                )
            out[place[0] + row, pl.ds(place[1] + col + zero, 8), :] = value
        return carry

    lax.fori_loop(0, size[0], step, 0)


def prolong_into(out, place, add, source, start, size, line, zero):
    narrow = starts(size[1])
    wide = starts(2 * size[1])

    def step(row, carry):
        for col in narrow:
            value = source[start[0] + row, pl.ds(start[1] + col + zero, 8), :]
            line[pl.ds(2 * col, 8, stride=2), :] = value
            line[pl.ds(2 * col + 1, 8, stride=2), :] = value
        for col in wide:
            value = line[pl.ds(col + zero, 8), :]
            for half in range(2):
                at_row, at_col = place[0] + 2 * row + half, place[1] + col + zero
                out[at_row, pl.ds(at_col, 8), :] = add[at_row, pl.ds(at_col, 8), :] + value
        return carry

    lax.fori_loop(0, size[0], step, 0)


def clear(array):
    rows, cols = array.shape[0], array.shape[1]

    def step(row, carry):
        array[row] = jnp.zeros((cols, 128), jnp.float32)
        return carry

    lax.fori_loop(0, rows, step, 0)


def copy_block(out, out_at, source, source_at, size, zero):
    def body(row, col):
        out[out_at[0] + row, pl.ds(out_at[1] + col, 8), :] = source[
            source_at[0] + row, pl.ds(source_at[1] + col, 8), :
        ]

    each(size[0], size[1], zero, body)


def correlate(first, first_at, second, second_at, size, zero):
    def step(row, sums):
        sums = list(sums)
        for col in range(0, size[1], 8):
            here = first[first_at[0] + row, pl.ds(first_at[1] + col + zero, 8), :]
            moved = (from_above(here), here, from_below(here))
            for a in range(3):
                for b in range(3):
                    window = second[
                        second_at[0] + row + a - 1, pl.ds(second_at[1] + col + zero + (b - 1), 8), :
                    ]
                    for c in range(3):
                        t = 9 * a + 3 * b + c
                        sums[t] = sums[t] + moved[c] * window
        return tuple(sums)

    blank = tuple(jnp.zeros((8, 128), jnp.float32) for _ in range(27))
    return lax.fori_loop(0, size[0], step, blank)


def place_of(shape, mesh_shape, walls):
    gx, gy = lax.axis_index("gx"), lax.axis_index("gy")
    levels = []
    for height in range(LOCAL):
        rows, cols = shape[0] >> height, shape[1] >> height
        levels.append(
            Level(walls, gx * rows, gy * cols, rows * mesh_shape[0], cols * mesh_shape[1])
        )
    return levels


def down_kernel(shape, mesh_shape, flip, *refs):
    (stencils, mask, still, low_first, block, high_first, low_second, high_second) = refs[:8]
    (kept, kept_pre, right1, pre1, right2) = refs[8:13]
    (wide, pre, line) = refs[13:]
    zero = still[0]
    walls = [mask[f].astype(jnp.float32) for f in range(6)]
    fine, middle = place_of(shape, mesh_shape, walls)
    rows, cols = shape[0], shape[1]
    copy_block(wide, (0, RIM0), low_first, (0, 0), (RIM0, cols), zero)
    copy_block(wide, (RIM0, RIM0), block, (0, 0), (rows, cols), zero)
    copy_block(wide, (RIM0 + rows, RIM0), high_first, (0, 0), (RIM0, cols), zero)
    copy_block(wide, (0, 0), low_second, (0, 0), (rows + 2 * RIM0, RIM0), zero)
    copy_block(wide, (0, RIM0 + cols), high_second, (0, 0), (rows + 2 * RIM0, RIM0), zero)
    before = LEVELS if flip else 0
    weights = weights_of(stencils, before, flip)
    origin = (RIM0, RIM0)
    smooth_into(
        pre, wide, weights, fine, (1, 1), (rows + 2 * RIM0 - 2, cols + 2 * RIM0 - 2), origin, zero
    )
    rows1, cols1 = rows // 2, cols // 2
    restrict_into(
        right1, (0, 0), wide, pre, line, fine, middle,
        (RIM0 - 2 * RIM1, RIM0 - 2 * RIM1), (rows1 + 2 * RIM1, cols1 + 2 * RIM1), origin, zero,
        (RIM1, RIM1),
    )
    inner = (RIM0 - KEEP, RIM0 - KEEP)
    size = (rows + 2 * KEEP, cols + 2 * KEEP)
    copy_block(kept, (0, 0), wide, inner, size, zero)
    copy_block(kept_pre, (0, 0), pre, inner, size, zero)
    weights = weights_of(stencils, before + 1, flip)
    clear(pre1)
    origin = (RIM1, RIM1)
    smooth_into(
        pre1, right1, weights, middle, (1, 1), (rows1 + 2 * RIM1 - 2, cols1 + 2 * RIM1 - 2),
        origin, zero,
    )
    restrict_into(
        right2, (0, 0), right1, pre1, line, middle, None, origin, (rows1 // 2, cols1 // 2), origin,
        zero, None,
    )


def up_kernel(shape, mesh_shape, flip, *refs):
    (stencils, mask, still, gathered, kept, kept_pre, right1, pre1) = refs[:8]
    refs = refs[8:]
    if flip:
        (after0_fwd, kept_fwd, after1_fwd, right1_fwd), refs = refs[:4], refs[4:]
        slabs_fwd, refs = refs[:7], refs[7:]
        (answer, sums), refs = refs[:2], refs[2:]
        (after0, after1), refs = refs[:2], refs[2:]
    else:
        (target,), refs = refs[:1], refs[1:]
        (answer, error, after0, after1), refs = refs[:4], refs[4:]
        slabs_fwd = ()
        slabs, refs = refs[:7], refs[7:]
    (right2, mid2, after2, right3, mid3, after3, right4, mid4, rest1, rest2) = refs[:10]
    (mid1, result1, mid0, line) = refs[10:14]
    zero = still[0]
    walls = [mask[f].astype(jnp.float32) for f in range(6)]
    fine, middle = place_of(shape, mesh_shape, walls)
    gx, gy = lax.axis_index("gx"), lax.axis_index("gy")
    across, along = mesh_shape
    rows2, cols2 = shape[0] // 4, shape[1] // 4
    before, later = (LEVELS, 0) if flip else (0, LEVELS)
    origin = (ROWS, COLS)
    for array in (right2, mid2, after2, right3, mid3, after3, right4, mid4, rest1, rest2):
        clear(array)

    def fill(peer, carry):
        for other in range(along):
            for row in range(rows2):
                for col in range(0, cols2, 8):
                    right2[
                        ROWS + peer * rows2 + row, pl.ds(COLS + other * cols2 + col, 8), :
                    ] = gathered[peer * along + other, row, pl.ds(col, 8), :]
        return carry

    lax.fori_loop(0, across, fill, 0)
    grids = []
    for height in range(LOCAL, LEVELS + 1):
        total = ((shape[0] * across) >> height, (shape[1] * along) >> height)
        grids.append(Level(walls, 0, 0, *total))
    arrays = ((right2, mid2, after2), (right3, mid3, after3))
    coarser = (right3, right4)
    for step in range(2):
        right, mid, after = arrays[step]
        level = grids[step]
        weights = weights_of(stencils, before + LOCAL + step, flip)
        smooth_into(mid, right, weights, level, origin, level.total, origin, zero, masked=False)
        half = (level.total[0] // 2, level.total[1] // 2)
        restrict_into(
            coarser[step], origin, right, mid, line, level, None, origin, half, origin, zero, None
        )
    level = grids[2]
    weights = weights_of(stencils, 2 * LEVELS, flip)
    smooth_into(mid4, right4, weights, level, origin, level.total, origin, zero, masked=False)
    for rest in (rest1, rest2):
        remain_into(rest, right4, mid4, level, origin, level.total, origin, zero, masked=False)
        smooth_into(
            mid4, rest, weights, level, origin, level.total, origin, zero, masked=False, add=mid4
        )
    below = mid4
    for step in (1, 0):
        right, mid, after = arrays[step]
        level = grids[step]
        prolong_into(mid, origin, mid, below, origin, grids[step + 1].total, line, zero)
        remain_into(after, right, mid, level, origin, level.total, origin, zero, masked=False)
        weights = weights_of(stencils, later + LOCAL + step, flip)
        smooth_into(
            mid, after, weights, level, origin, level.total, origin, zero, masked=False, add=mid
        )
        below = mid
    rows1, cols1 = shape[0] // 2, shape[1] // 2
    half = RIM1 // 2
    prolong_into(
        mid1, (0, 0), pre1, below,
        (ROWS + gx * rows2 - half, COLS + gy * cols2 - half),
        (rows2 + 2 * half, cols2 + 2 * half), line, zero,
    )
    origin = (RIM1, RIM1)
    remain_into(
        after1, right1, mid1, middle, (2, 2), (rows1 + 2 * RIM1 - 4, cols1 + 2 * RIM1 - 4),
        origin, zero,
    )
    weights = weights_of(stencils, later + 1, flip)
    smooth_into(
        result1, after1, weights, middle, (3, 3), (rows1 + 2 * RIM1 - 6, cols1 + 2 * RIM1 - 6),
        origin, zero, add=mid1,
    )
    rows, cols = shape[0], shape[1]
    prolong_into(mid0, (0, 0), kept_pre, result1, (3, 3), (rows1 + 2, cols1 + 2), line, zero)
    origin = (KEEP, KEEP)
    remain_into(after0, kept, mid0, fine, (1, 1), (rows + 2, cols + 2), origin, zero)
    weights = weights_of(stencils, later, flip)

    def finish(row, col):
        value = smoothed(after0, weights, row + KEEP, col + KEEP)
        value = value + mid0[row + KEEP, pl.ds(col + KEEP, 8), :]
        answer[row, pl.ds(col, 8), :] = value
        if not flip:
            error[row, pl.ds(col, 8), :] = value - target[row, pl.ds(col, 8), :]

    each(rows, cols, zero, finish)
    kept_arrays = (
        (right2, grids[0]), (after2, grids[0]), (right3, grids[1]), (after3, grids[1]),
        (right4, grids[2]), (rest1, grids[2]), (rest2, grids[2]),
    )

    def own(level):
        return level.total[0] // across

    if not flip:
        for slab, (array, level) in zip(slabs, kept_arrays):
            count = own(level)
            for row in range(count + 2):
                slab[row] = array[ROWS - 1 + gx * count + row]
        return
    chosen = jnp.where(gy == 0, 1.0, 0.0)

    def write(row, sums27, scale):
        for t in range(27):
            line[pl.ds(t, 1), :] = jnp.sum(sums27[t], axis=0, keepdims=True)
        ones = jnp.ones((8, 128), jnp.float32)
        total = lax.dot_general(
            ones, line[0:32, :], (((1,), (1,)), ((), ())),
            precision=lax.Precision.HIGHEST, preferred_element_type=jnp.float32,
        )
        sums[row : row + 1, :] = scale * total[0:1, 0:27]

    line[0:32, :] = jnp.zeros((32, 128), jnp.float32)
    mine = (KEEP, KEEP)
    write(LEVELS, correlate(kept, mine, after0_fwd, mine, (rows, cols), zero), 1.0)
    write(0, correlate(after0, mine, kept_fwd, mine, (rows, cols), zero), 1.0)
    mine = (RIM1, RIM1)
    write(LEVELS + 1, correlate(right1, mine, after1_fwd, mine, (rows1, cols1), zero), 4.0)
    write(1, correlate(after1, mine, right1_fwd, mine, (rows1, cols1), zero), 4.0)
    scale = 16.0
    for step in range(2):
        level = grids[step]
        right, mid, after = arrays[step]
        count = own(level)
        start = (ROWS + gx * count, COLS)
        size = (count, level.total[1])
        slab_right, slab_after = slabs_fwd[2 * step], slabs_fwd[2 * step + 1]
        found = correlate(right, start, slab_after, (1, COLS), size, zero)
        write(LEVELS + LOCAL + step, found, chosen * scale)
        found = correlate(after, start, slab_right, (1, COLS), size, zero)
        write(LOCAL + step, found, chosen * scale)
        scale *= 4.0
    level = grids[2]
    count = own(level)
    start = (ROWS + gx * count, COLS)
    size = (count, level.total[1])
    found = None
    for array, slab in ((right4, slabs_fwd[6]), (rest1, slabs_fwd[5]), (rest2, slabs_fwd[4])):
        more = correlate(array, start, slab, (1, COLS), size, zero)
        found = more if found is None else [x + y for x, y in zip(found, more)]
    write(2 * LEVELS, found, chosen * scale)


def spaces(count_smem, arrays):
    smem = [pl.BlockSpec(memory_space=pltpu.SMEM)] * count_smem
    return smem + [pl.BlockSpec(memory_space=pltpu.VMEM)] * (len(arrays) - count_smem)


def call(kernel, outs, scratch, arrays, name):
    return pl.pallas_call(
        kernel,
        out_shape=[jax.ShapeDtypeStruct(shape, jnp.float32) for shape in outs],
        in_specs=spaces(3, arrays),
        out_specs=[pl.BlockSpec(memory_space=pltpu.VMEM)] * len(outs),
        scratch_shapes=[pltpu.VMEM(shape, jnp.float32) for shape in scratch],
        compiler_params=pltpu.CompilerParams(vmem_limit_bytes=60 * 2**20),
        name=name,
    )(*arrays)


def shift_pair(low_part, high_part, axis):
    peers = lax.axis_size(axis)
    up = [(i, i + 1) for i in range(peers - 1)]
    down = [(j, i) for i, j in up]
    return lax.ppermute(high_part, axis, up), lax.ppermute(low_part, axis, down)


def rim(block):
    rows, cols = block.shape[0], block.shape[1]
    low_first, high_first = shift_pair(block[:RIM0], block[rows - RIM0 :], "gx")
    tall_low = jnp.concatenate([low_first[:, :RIM0], block[:, :RIM0], high_first[:, :RIM0]], 0)
    tall_high = jnp.concatenate(
        [low_first[:, cols - RIM0 :], block[:, cols - RIM0 :], high_first[:, cols - RIM0 :]], 0
    )
    low_second, high_second = shift_pair(tall_low, tall_high, "gy")
    return [low_first, block, high_first, low_second, high_second]


def share(block):
    peers = lax.axis_size("gx") * lax.axis_size("gy")
    copies = jnp.broadcast_to(block[None], (peers,) + block.shape)
    return lax.all_to_all(copies, PEERS, 0, 0, tiled=True)


def on_device(rhs, target, stencils, face_mask):
    shape = rhs.shape
    mesh_shape = (lax.axis_size("gx"), lax.axis_size("gy"))
    rows, cols = shape[0], shape[1]
    still = jnp.zeros((1,), jnp.int32)
    small = [stencils, face_mask, still]
    wide = (rows + 2 * RIM0, cols + 2 * RIM0, 128)
    kept = (rows + 2 * KEEP, cols + 2 * KEEP, 128)
    wide1 = (rows // 2 + 2 * RIM1, cols // 2 + 2 * RIM1, 128)
    own2 = (rows // 4, cols // 4, 128)
    totals = [
        ((rows * mesh_shape[0]) >> h, (cols * mesh_shape[1]) >> h) for h in range(LOCAL, LEVELS + 1)
    ]
    whole = [(a + 2 * ROWS, b + 2 * COLS, 128) for a, b in totals]
    slab = [(a // mesh_shape[0] + 2, b + 2 * COLS, 128) for a, b in totals]
    slabs = [slab[0], slab[0], slab[1], slab[1], slab[2], slab[2], slab[2]]
    line = (max(totals[0][1], wide[1], 64), 128)
    scratch = [whole[0]] * 3 + [whole[1]] * 3 + [whole[2]] * 4 + [wide1, wide1, kept, line]

    def down(block, flip):
        return call(
            functools.partial(down_kernel, shape, mesh_shape, flip),
            [kept, kept, wide1, wide1, own2], [wide, wide, line], small + rim(block),
            "down_back" if flip else "down",
        )

    keep0, pre0, right1, pre1, right2 = down(rhs, False)
    answer, error, after0, after1, *kept_slabs = call(
        functools.partial(up_kernel, shape, mesh_shape, False),
        [shape, shape, kept, wide1] + slabs, scratch,
        small + [share(right2), keep0, pre0, right1, pre1, target], "up",
    )
    back0, back_pre0, back1, back_pre1, back2 = down(error, True)
    grad_rhs, sums = call(
        functools.partial(up_kernel, shape, mesh_shape, True),
        [shape, (2 * LEVELS + 1, 27)], [kept, wide1] + scratch,
        small + [share(back2), back0, back_pre0, back1, back_pre1]
        + [after0, keep0, after1, right1] + list(kept_slabs), "up_back",
    )
    cells = rows * mesh_shape[0] * cols * mesh_shape[1] * shape[2]
    grads = jnp.sum(share(sums), axis=0) / cells
    return answer, grad_rhs, grads


def solution(mesh):
    placed = (P("gx", "gy", None), P("gx", "gy", None), P(), P())
    return jax.shard_map(
        on_device,
        mesh=mesh,
        in_specs=placed,
        out_specs=(P("gx", "gy", None), P("gx", "gy", None), P()),
        check_vma=False,
    )
```

```python
import functools

import jax
import jax.numpy as jnp
from jax import lax
from jax.experimental import pallas as pl
from jax.experimental.pallas import tpu as pltpu
from jax.sharding import PartitionSpec as P

LEVELS = 4
SWEEPS = 3
LOCAL = 2
RIM0 = 10
RIM1 = 4
KEEP = 2
ROWS, COLS = 2, 8
PEERS = ("gx", "gy")
SLOTS = 4
BODY = 48
NEAR = 2**21


def starts(width):
    places = list(range(0, width - 7, 8))
    if width % 8:
        places.append(width - 8)
    return places


def lanes(shape=(8, 128)):
    return lax.broadcasted_iota(jnp.int32, shape, 1)


def sublanes(shape=(8, 128)):
    return lax.broadcasted_iota(jnp.int32, shape, 0)


def from_below(value):
    return jnp.where(lanes(value.shape) == 0, 0.0, pltpu.roll(value, 1, 1))


def from_above(value):
    last = value.shape[1] - 1
    return jnp.where(lanes(value.shape) == last, 0.0, pltpu.roll(value, last, 1))


def weights_of(stencils, row, flip):
    return [stencils[row, 26 - t if flip else t] for t in range(27)]


class Level:
    def __init__(self, walls, first, second, total_first, total_second):
        self.walls = walls
        self.first = first
        self.second = second
        self.total = (total_first, total_second)

    def row_wall(self, row):
        at = self.first + row
        return jnp.where(at == 0, self.walls[0], 0.0) + jnp.where(
            at == self.total[0] - 1, self.walls[1], 0.0
        )

    def row_inside(self, row):
        at = self.first + row
        return (at >= 0) & (at < self.total[0])

    def wall_plane(self, col):
        at = self.second + col + sublanes()
        lane = lanes()
        plane = jnp.where(at == 0, self.walls[2], 0.0)
        plane = plane + jnp.where(at == self.total[1] - 1, self.walls[3], 0.0)
        plane = plane + jnp.where(lane == 0, self.walls[4], 0.0)
        return plane + jnp.where(lane == 127, self.walls[5], 0.0)

    def inside(self, row, col):
        at = self.second + col + sublanes()
        return self.row_inside(row) & (at >= 0) & (at < self.total[1])


def smoothed(source, weights, row, col):
    sums = [None, None, None]
    for a in range(3):
        for b in range(3):
            window = source[row + (a - 1), pl.ds(col + (b - 1), 8), :]
            for c in range(3):
                term = weights[9 * a + 3 * b + c] * window
                sums[c] = term if sums[c] is None else sums[c] + term
    return sums[1] + from_below(sums[0]) + from_above(sums[2])


def applied(source, level, row, col, at_row, at_col):
    here = source[row, pl.ds(col, 8), :]
    beside = source[row - 1, pl.ds(col, 8), :] + source[row + 1, pl.ds(col, 8), :]
    beside = beside + source[row, pl.ds(col - 1, 8), :] + source[row, pl.ds(col + 1, 8), :]
    beside = beside + from_below(here) + from_above(here)
    diagonal = (6.0 - level.row_wall(at_row)) - level.wall_plane(at_col)
    return diagonal * here - beside


def rows_at_once(rows, chunks):
    return max(n for n in range(1, rows + 1) if rows % n == 0 and (n == 1 or n * chunks <= BODY))


def by_rows(rows, chunks, step):
    count = rows_at_once(rows, chunks)

    def several(turn, carry):
        for row in range(count):
            step(turn * count + row, row % SLOTS)
        return carry

    lax.fori_loop(0, rows // count, several, 0)


def each(rows, cols, zero, body):
    places = starts(cols)

    def step(row, slot):
        for place in places:
            body(row, zero + place)

    by_rows(rows, len(places), step)


def smooth_into(out, source, weights, level, start, size, origin, zero, masked=True, add=None):
    def body(row, col):
        row, col = row + start[0], col + start[1]
        value = smoothed(source, weights, row, col)
        if masked:
            value = jnp.where(level.inside(row - origin[0], col - origin[1]), value, 0.0)
        if add is not None:
            value = value + add[row, pl.ds(col, 8), :]
        out[row, pl.ds(col, 8), :] = value

    each(size[0], size[1], zero, body)


def remain_into(out, right, source, level, start, size, origin, zero, masked=True):
    def body(row, col):
        row, col = row + start[0], col + start[1]
        value = right[row, pl.ds(col, 8), :] - applied(
            source, level, row, col, row - origin[0], col - origin[1]
        )
        if masked:
            value = jnp.where(level.inside(row - origin[0], col - origin[1]), value, 0.0)
        out[row, pl.ds(col, 8), :] = value

    each(size[0], size[1], zero, body)


def restrict_into(out, place, right, source, line, fine, coarse, start, size, origin, zero, masked):
    wide = starts(2 * size[1])
    narrow = starts(size[1])

    def step(row, slot):
        for col in wide:
            col = col + zero
            total = None
            for half in range(2):
                at_row, at_col = start[0] + 2 * row + half, start[1] + col
                value = right[at_row, pl.ds(at_col, 8), :] - applied(
                    source, fine, at_row, at_col, at_row - origin[0], at_col - origin[1]
                )
                total = value if total is None else total + value
            line[slot, pl.ds(col, 8), :] = total
        for col in narrow:
            value = line[slot, pl.ds(2 * col, 8, stride=2), :]
            value = value + line[slot, pl.ds(2 * col + 1, 8, stride=2), :]
            value = 0.25 * value
            if masked is not None:
                value = jnp.where(
                    coarse.inside(place[0] + row - masked[0], place[1] + col + zero - masked[1]),
                    value,
                    0.0,
                )
            out[place[0] + row, pl.ds(place[1] + col + zero, 8), :] = value

    by_rows(size[0], 2 * len(wide), step)


def prolong_into(out, place, add, source, start, size, line, zero):
    narrow = starts(size[1])
    wide = starts(2 * size[1])

    def step(row, slot):
        for col in narrow:
            value = source[start[0] + row, pl.ds(start[1] + col + zero, 8), :]
            line[slot, pl.ds(2 * col, 8, stride=2), :] = value
            line[slot, pl.ds(2 * col + 1, 8, stride=2), :] = value
        for col in wide:
            value = line[slot, pl.ds(col + zero, 8), :]
            for half in range(2):
                at_row, at_col = place[0] + 2 * row + half, place[1] + col + zero
                out[at_row, pl.ds(at_col, 8), :] = add[at_row, pl.ds(at_col, 8), :] + value

    by_rows(size[0], len(wide), step)


def clear(array):
    rows, cols = array.shape[0], array.shape[1]

    def step(row, slot):
        array[row] = jnp.zeros((cols, 128), jnp.float32)

    by_rows(rows, cols // 8, step)


def copy_block(out, out_at, source, source_at, size, zero):
    def body(row, col):
        out[out_at[0] + row, pl.ds(out_at[1] + col, 8), :] = source[
            source_at[0] + row, pl.ds(source_at[1] + col, 8), :
        ]

    each(size[0], size[1], zero, body)


def correlate(first, first_at, second, second_at, size, zero):
    cols = range(0, size[1], 8)
    count = rows_at_once(size[0], len(cols))

    def step(turn, sums):
        sums = list(sums)
        for row, col in [(turn * count + more, col) for more in range(count) for col in cols]:
            here = first[first_at[0] + row, pl.ds(first_at[1] + col + zero, 8), :]
            moved = (from_above(here), here, from_below(here))
            for a in range(3):
                for b in range(3):
                    window = second[
                        second_at[0] + row + a - 1, pl.ds(second_at[1] + col + zero + (b - 1), 8), :
                    ]
                    for c in range(3):
                        t = 9 * a + 3 * b + c
                        sums[t] = sums[t] + moved[c] * window
        return tuple(sums)

    blank = tuple(jnp.zeros((8, 128), jnp.float32) for _ in range(27))
    return lax.fori_loop(0, size[0] // count, step, blank)


def place_of(shape, mesh_shape, walls):
    gx, gy = lax.axis_index("gx"), lax.axis_index("gy")
    levels = []
    for height in range(LOCAL):
        rows, cols = shape[0] >> height, shape[1] >> height
        levels.append(
            Level(walls, gx * rows, gy * cols, rows * mesh_shape[0], cols * mesh_shape[1])
        )
    return levels


def down_kernel(shape, mesh_shape, flip, *refs):
    (stencils, mask, still, low_first, block, high_first, low_second, high_second) = refs[:8]
    (kept, kept_pre, right1, pre1, right2) = refs[8:13]
    (wide, pre, line) = refs[13:]
    zero = still[0]
    walls = [mask[f].astype(jnp.float32) for f in range(6)]
    fine, middle = place_of(shape, mesh_shape, walls)
    rows, cols = shape[0], shape[1]
    copy_block(wide, (0, RIM0), low_first, (0, 0), (RIM0, cols), zero)
    copy_block(wide, (RIM0, RIM0), block, (0, 0), (rows, cols), zero)
    copy_block(wide, (RIM0 + rows, RIM0), high_first, (0, 0), (RIM0, cols), zero)
    copy_block(wide, (0, 0), low_second, (0, 0), (rows + 2 * RIM0, RIM0), zero)
    copy_block(wide, (0, RIM0 + cols), high_second, (0, 0), (rows + 2 * RIM0, RIM0), zero)
    before = LEVELS if flip else 0
    weights = weights_of(stencils, before, flip)
    origin = (RIM0, RIM0)
    smooth_into(
        pre, wide, weights, fine, (1, 1), (rows + 2 * RIM0 - 2, cols + 2 * RIM0 - 2), origin, zero
    )
    rows1, cols1 = rows // 2, cols // 2
    restrict_into(
        right1, (0, 0), wide, pre, line, fine, middle,
        (RIM0 - 2 * RIM1, RIM0 - 2 * RIM1), (rows1 + 2 * RIM1, cols1 + 2 * RIM1), origin, zero,
        (RIM1, RIM1),
    )
    inner = (RIM0 - KEEP, RIM0 - KEEP)
    size = (rows + 2 * KEEP, cols + 2 * KEEP)
    copy_block(kept, (0, 0), wide, inner, size, zero)
    copy_block(kept_pre, (0, 0), pre, inner, size, zero)
    weights = weights_of(stencils, before + 1, flip)
    clear(pre1)
    origin = (RIM1, RIM1)
    smooth_into(
        pre1, right1, weights, middle, (1, 1), (rows1 + 2 * RIM1 - 2, cols1 + 2 * RIM1 - 2),
        origin, zero,
    )
    restrict_into(
        right2, (0, 0), right1, pre1, line, middle, None, origin, (rows1 // 2, cols1 // 2), origin,
        zero, None,
    )


def up_kernel(shape, mesh_shape, flip, *refs):
    (stencils, mask, still, gathered, kept, kept_pre, right1, pre1) = refs[:8]
    refs = refs[8:]
    if flip:
        (after0_fwd, kept_fwd, after1_fwd, right1_fwd), refs = refs[:4], refs[4:]
        slabs_fwd, refs = refs[:7], refs[7:]
        (answer, sums), refs = refs[:2], refs[2:]
        (after0, after1), refs = refs[:2], refs[2:]
    else:
        (target,), refs = refs[:1], refs[1:]
        (answer, error, after0, after1), refs = refs[:4], refs[4:]
        slabs_fwd = ()
        slabs, refs = refs[:7], refs[7:]
    (right2, mid2, after2, right3, mid3, after3, right4, mid4, rest1, rest2) = refs[:10]
    (mid1, result1, mid0, line) = refs[10:14]
    zero = still[0]
    walls = [mask[f].astype(jnp.float32) for f in range(6)]
    fine, middle = place_of(shape, mesh_shape, walls)
    gx, gy = lax.axis_index("gx"), lax.axis_index("gy")
    across, along = mesh_shape
    rows2, cols2 = shape[0] // 4, shape[1] // 4
    before, later = (LEVELS, 0) if flip else (0, LEVELS)
    origin = (ROWS, COLS)
    for array in (right2, mid2, after2, right3, mid3, after3, right4, mid4, rest1, rest2):
        clear(array)

    def fill(peer, carry):
        for other in range(along):
            for row in range(rows2):
                for col in range(0, cols2, 8):
                    right2[
                        ROWS + peer * rows2 + row, pl.ds(COLS + other * cols2 + col, 8), :
                    ] = gathered[peer * along + other, row, pl.ds(col, 8), :]
        return carry

    lax.fori_loop(0, across, fill, 0)
    grids = []
    for height in range(LOCAL, LEVELS + 1):
        total = ((shape[0] * across) >> height, (shape[1] * along) >> height)
        grids.append(Level(walls, 0, 0, *total))
    arrays = ((right2, mid2, after2), (right3, mid3, after3))
    coarser = (right3, right4)
    for step in range(2):
        right, mid, after = arrays[step]
        level = grids[step]
        weights = weights_of(stencils, before + LOCAL + step, flip)
        smooth_into(mid, right, weights, level, origin, level.total, origin, zero, masked=False)
        half = (level.total[0] // 2, level.total[1] // 2)
        restrict_into(
            coarser[step], origin, right, mid, line, level, None, origin, half, origin, zero, None
        )
    level = grids[2]
    weights = weights_of(stencils, 2 * LEVELS, flip)
    smooth_into(mid4, right4, weights, level, origin, level.total, origin, zero, masked=False)
    for rest in (rest1, rest2):
        remain_into(rest, right4, mid4, level, origin, level.total, origin, zero, masked=False)
        smooth_into(
            mid4, rest, weights, level, origin, level.total, origin, zero, masked=False, add=mid4
        )
    below = mid4
    for step in (1, 0):
        right, mid, after = arrays[step]
        level = grids[step]
        prolong_into(mid, origin, mid, below, origin, grids[step + 1].total, line, zero)
        remain_into(after, right, mid, level, origin, level.total, origin, zero, masked=False)
        weights = weights_of(stencils, later + LOCAL + step, flip)
        smooth_into(
            mid, after, weights, level, origin, level.total, origin, zero, masked=False, add=mid
        )
        below = mid
    rows1, cols1 = shape[0] // 2, shape[1] // 2
    half = RIM1 // 2
    prolong_into(
        mid1, (0, 0), pre1, below,
        (ROWS + gx * rows2 - half, COLS + gy * cols2 - half),
        (rows2 + 2 * half, cols2 + 2 * half), line, zero,
    )
    origin = (RIM1, RIM1)
    remain_into(
        after1, right1, mid1, middle, (2, 2), (rows1 + 2 * RIM1 - 4, cols1 + 2 * RIM1 - 4),
        origin, zero,
    )
    weights = weights_of(stencils, later + 1, flip)
    smooth_into(
        result1, after1, weights, middle, (3, 3), (rows1 + 2 * RIM1 - 6, cols1 + 2 * RIM1 - 6),
        origin, zero, add=mid1,
    )
    rows, cols = shape[0], shape[1]
    prolong_into(mid0, (0, 0), kept_pre, result1, (3, 3), (rows1 + 2, cols1 + 2), line, zero)
    origin = (KEEP, KEEP)
    remain_into(after0, kept, mid0, fine, (1, 1), (rows + 2, cols + 2), origin, zero)
    weights = weights_of(stencils, later, flip)

    def finish(row, col):
        value = smoothed(after0, weights, row + KEEP, col + KEEP)
        value = value + mid0[row + KEEP, pl.ds(col + KEEP, 8), :]
        answer[row, pl.ds(col, 8), :] = value
        if not flip:
            error[row, pl.ds(col, 8), :] = value - target[row, pl.ds(col, 8), :]

    each(rows, cols, zero, finish)
    kept_arrays = (
        (right2, grids[0]), (after2, grids[0]), (right3, grids[1]), (after3, grids[1]),
        (right4, grids[2]), (rest1, grids[2]), (rest2, grids[2]),
    )

    def own(level):
        return level.total[0] // across

    if not flip:
        for slab, (array, level) in zip(slabs, kept_arrays):
            count = own(level)
            for row in range(count + 2):
                slab[row] = array[ROWS - 1 + gx * count + row]
        return
    chosen = jnp.where(gy == 0, 1.0, 0.0)

    (part,) = refs[14:]

    def write(row, found, scale):
        for t in range(27):
            part[pl.ds(8 * (32 * row + t), 8), :] = scale * found[t]
        for t in range(27, 32):
            part[pl.ds(8 * (32 * row + t), 8), :] = jnp.zeros((8, 128), jnp.float32)

    mine = (KEEP, KEEP)
    write(LEVELS, correlate(kept, mine, after0_fwd, mine, (rows, cols), zero), 1.0)
    write(0, correlate(after0, mine, kept_fwd, mine, (rows, cols), zero), 1.0)
    mine = (RIM1, RIM1)
    write(LEVELS + 1, correlate(right1, mine, after1_fwd, mine, (rows1, cols1), zero), 4.0)
    write(1, correlate(after1, mine, right1_fwd, mine, (rows1, cols1), zero), 4.0)
    scale = 16.0
    for step in range(2):
        level = grids[step]
        right, mid, after = arrays[step]
        count = own(level)
        start = (ROWS + gx * count, COLS)
        size = (count, level.total[1])
        slab_right, slab_after = slabs_fwd[2 * step], slabs_fwd[2 * step + 1]
        found = correlate(right, start, slab_after, (1, COLS), size, zero)
        write(LEVELS + LOCAL + step, found, chosen * scale)
        found = correlate(after, start, slab_right, (1, COLS), size, zero)
        write(LOCAL + step, found, chosen * scale)
        scale *= 4.0
    level = grids[2]
    count = own(level)
    start = (ROWS + gx * count, COLS)
    size = (count, level.total[1])
    found = None
    for array, slab in ((right4, slabs_fwd[6]), (rest1, slabs_fwd[5]), (rest2, slabs_fwd[4])):
        more = correlate(array, start, slab, (1, COLS), size, zero)
        found = more if found is None else [x + y for x, y in zip(found, more)]
    write(2 * LEVELS, found, chosen * scale)
    ones = jnp.ones((8, 128), jnp.float32)
    for row in range(2 * LEVELS + 1):
        folded = None
        for fold in range(8):
            more = part[pl.ds(8 * 32 * row + fold, 32, stride=8), :]
            folded = more if folded is None else folded + more
        total = lax.dot_general(
            ones, folded, (((1,), (1,)), ((), ())),
            precision=lax.Precision.HIGHEST, preferred_element_type=jnp.float32,
        )
        sums[row : row + 1, :] = total[0:1, 0:27]


def spaces(count_smem, arrays):
    smem = [pl.BlockSpec(memory_space=pltpu.SMEM)] * count_smem
    return smem + [pl.BlockSpec(memory_space=pltpu.VMEM)] * (len(arrays) - count_smem)


def padded(shape):
    whole = 4 * -(-shape[-1] // 128) * 128 * -(-shape[-2] // 8) * 8
    for size in shape[:-2]:
        whole *= size
    return whole


def near_enough(arrays):
    return max(padded(x.shape) for x in arrays[3:]) <= NEAR


def call(kernel, outs, scratch, arrays, name, far=()):
    arrays = list(arrays)
    near = near_enough(arrays)
    if near:
        arrays[3:] = [pltpu.with_memory_space_constraint(x, pltpu.VMEM) for x in arrays[3:]]
    made = [
        pltpu.VMEM(shape, jnp.float32)
        if near and place not in far
        else jax.ShapeDtypeStruct(shape, jnp.float32)
        for place, shape in enumerate(outs)
    ]
    held = sum(padded(shape) for shape in list(outs) + list(scratch))
    held += sum(padded(x.shape) for x in arrays[3:])
    return pl.pallas_call(
        kernel,
        out_shape=made,
        in_specs=spaces(3, arrays),
        out_specs=[pl.BlockSpec(memory_space=pltpu.VMEM)] * len(outs),
        scratch_shapes=[pltpu.VMEM(shape, jnp.float32) for shape in scratch],
        compiler_params=pltpu.CompilerParams(vmem_limit_bytes=min(60 * 2**20, held + 4 * 2**20)),
        name=name,
    )(*arrays)


def shift_pair(low_part, high_part, axis):
    peers = lax.axis_size(axis)
    up = [(i, i + 1) for i in range(peers - 1)]
    down = [(j, i) for i, j in up]
    return lax.ppermute(high_part, axis, up), lax.ppermute(low_part, axis, down)


def rim(block):
    rows, cols = block.shape[0], block.shape[1]
    low_first, high_first = shift_pair(block[:RIM0], block[rows - RIM0 :], "gx")
    tall_low = jnp.concatenate([low_first[:, :RIM0], block[:, :RIM0], high_first[:, :RIM0]], 0)
    tall_high = jnp.concatenate(
        [low_first[:, cols - RIM0 :], block[:, cols - RIM0 :], high_first[:, cols - RIM0 :]], 0
    )
    low_second, high_second = shift_pair(tall_low, tall_high, "gy")
    return [low_first, block, high_first, low_second, high_second]


def share(block):
    peers = lax.axis_size("gx") * lax.axis_size("gy")
    copies = jnp.broadcast_to(block[None], (peers,) + block.shape)
    return lax.all_to_all(copies, PEERS, 0, 0, tiled=True)


def on_device(rhs, target, stencils, face_mask):
    shape = rhs.shape
    mesh_shape = (lax.axis_size("gx"), lax.axis_size("gy"))
    rows, cols = shape[0], shape[1]
    still = jnp.zeros((1,), jnp.int32)
    small = [stencils, face_mask, still]
    wide = (rows + 2 * RIM0, cols + 2 * RIM0, 128)
    kept = (rows + 2 * KEEP, cols + 2 * KEEP, 128)
    wide1 = (rows // 2 + 2 * RIM1, cols // 2 + 2 * RIM1, 128)
    own2 = (rows // 4, cols // 4, 128)
    totals = [
        ((rows * mesh_shape[0]) >> h, (cols * mesh_shape[1]) >> h) for h in range(LOCAL, LEVELS + 1)
    ]
    whole = [(a + 2 * ROWS, b + 2 * COLS, 128) for a, b in totals]
    slab = [(a // mesh_shape[0] + 2, b + 2 * COLS, 128) for a, b in totals]
    slabs = [slab[0], slab[0], slab[1], slab[1], slab[2], slab[2], slab[2]]
    line = (SLOTS, -(-max(totals[0][1], wide[1]) // 8) * 8, 128)
    part = ((2 * LEVELS + 1) * 32 * 8, 128)
    scratch = [whole[0]] * 3 + [whole[1]] * 3 + [whole[2]] * 4 + [wide1, wide1, kept, line]

    def down(block, flip):
        return call(
            functools.partial(down_kernel, shape, mesh_shape, flip),
            [kept, kept, wide1, wide1, own2], [wide, wide, line], small + rim(block),
            "down_back" if flip else "down",
        )

    keep0, pre0, right1, pre1, right2 = down(rhs, False)
    answer, error, after0, after1, *kept_slabs = call(
        functools.partial(up_kernel, shape, mesh_shape, False),
        [shape, shape, kept, wide1] + slabs, scratch,
        small + [share(right2), keep0, pre0, right1, pre1, target], "up", (0,),
    )
    back0, back_pre0, back1, back_pre1, back2 = down(error, True)
    grad_rhs, sums = call(
        functools.partial(up_kernel, shape, mesh_shape, True),
        [shape, (2 * LEVELS + 1, 27)], [kept, wide1] + scratch + [part],
        small + [share(back2), back0, back_pre0, back1, back_pre1]
        + [after0, keep0, after1, right1] + list(kept_slabs), "up_back", (0,),
    )
    cells = rows * mesh_shape[0] * cols * mesh_shape[1] * shape[2]
    grads = jnp.sum(share(sums), axis=0) / cells
    return answer, grad_rhs, grads


def solution(mesh):
    placed = (P("gx", "gy", None), P("gx", "gy", None), P(), P())
    return jax.shard_map(
        on_device,
        mesh=mesh,
        in_specs=placed,
        out_specs=(P("gx", "gy", None), P("gx", "gy", None), P()),
        check_vma=False,
    )
```

```python
import functools

import jax
import jax.numpy as jnp
from jax import lax
from jax.experimental import pallas as pl
from jax.experimental.pallas import tpu as pltpu
from jax.sharding import PartitionSpec as P

LEVELS = 4
SWEEPS = 3
LOCAL = 2
RIM0 = 10
RIM1 = 4
KEEP = 2
ROWS, COLS = 2, 8
SECOND = ("y", "core")
PEERS = ("gx",) + SECOND
SLOTS = 4
BODY = 64
NEAR = 2**21


def second_index():
    return lax.axis_index("y") * lax.axis_size("core") + lax.axis_index("core")


def second_size():
    return lax.axis_size("y") * lax.axis_size("core")


def starts(width):
    places = list(range(0, width - 7, 8))
    if width % 8:
        places.append(width - 8)
    return places


def lanes(shape=(8, 128)):
    return lax.broadcasted_iota(jnp.int32, shape, 1)


def sublanes(shape=(8, 128)):
    return lax.broadcasted_iota(jnp.int32, shape, 0)


def from_below(value):
    return jnp.where(lanes(value.shape) == 0, 0.0, pltpu.roll(value, 1, 1))


def from_above(value):
    last = value.shape[1] - 1
    return jnp.where(lanes(value.shape) == last, 0.0, pltpu.roll(value, last, 1))


def weights_of(stencils, row, flip):
    return [stencils[row, 26 - t if flip else t] for t in range(27)]


class Level:
    def __init__(self, walls, first, second, total_first, total_second):
        self.walls = walls
        self.first = first
        self.second = second
        self.total = (total_first, total_second)

    def row_wall(self, row):
        at = self.first + row
        return jnp.where(at == 0, self.walls[0], 0.0) + jnp.where(
            at == self.total[0] - 1, self.walls[1], 0.0
        )

    def row_inside(self, row):
        at = self.first + row
        return (at >= 0) & (at < self.total[0])

    def wall_plane(self, col):
        at = self.second + col + sublanes()
        lane = lanes()
        plane = jnp.where(at == 0, self.walls[2], 0.0)
        plane = plane + jnp.where(at == self.total[1] - 1, self.walls[3], 0.0)
        plane = plane + jnp.where(lane == 0, self.walls[4], 0.0)
        return plane + jnp.where(lane == 127, self.walls[5], 0.0)

    def inside(self, row, col):
        at = self.second + col + sublanes()
        return self.row_inside(row) & (at >= 0) & (at < self.total[1])


def smoothed(source, weights, row, col):
    sums = [None, None, None]
    for a in range(3):
        for b in range(3):
            window = source[row + (a - 1), pl.ds(col + (b - 1), 8), :]
            for c in range(3):
                term = weights[9 * a + 3 * b + c] * window
                sums[c] = term if sums[c] is None else sums[c] + term
    return sums[1] + from_below(sums[0]) + from_above(sums[2])


def applied(source, level, row, col, at_row, at_col):
    here = source[row, pl.ds(col, 8), :]
    beside = source[row - 1, pl.ds(col, 8), :] + source[row + 1, pl.ds(col, 8), :]
    beside = beside + source[row, pl.ds(col - 1, 8), :] + source[row, pl.ds(col + 1, 8), :]
    beside = beside + from_below(here) + from_above(here)
    diagonal = (6.0 - level.row_wall(at_row)) - level.wall_plane(at_col)
    return diagonal * here - beside


def rows_at_once(rows, chunks):
    return max(n for n in range(1, rows + 1) if rows % n == 0 and (n == 1 or n * chunks <= BODY))


def by_rows(rows, chunks, step):
    count = rows_at_once(rows, chunks)

    def several(turn, carry):
        for row in range(count):
            step(turn * count + row, row % SLOTS)
        return carry

    lax.fori_loop(0, rows // count, several, 0)


def each(rows, cols, zero, body):
    places = starts(cols)

    def step(row, slot):
        for place in places:
            body(row, zero + place)

    by_rows(rows, len(places), step)


def smooth_into(out, source, weights, level, start, size, origin, zero, masked=True, add=None):
    def body(row, col):
        row, col = row + start[0], col + start[1]
        value = smoothed(source, weights, row, col)
        if masked:
            value = jnp.where(level.inside(row - origin[0], col - origin[1]), value, 0.0)
        if add is not None:
            value = value + add[row, pl.ds(col, 8), :]
        out[row, pl.ds(col, 8), :] = value

    each(size[0], size[1], zero, body)


def remain_into(out, right, source, level, start, size, origin, zero, masked=True):
    def body(row, col):
        row, col = row + start[0], col + start[1]
        value = right[row, pl.ds(col, 8), :] - applied(
            source, level, row, col, row - origin[0], col - origin[1]
        )
        if masked:
            value = jnp.where(level.inside(row - origin[0], col - origin[1]), value, 0.0)
        out[row, pl.ds(col, 8), :] = value

    each(size[0], size[1], zero, body)


def restrict_into(out, place, right, source, line, fine, coarse, start, size, origin, zero, masked):
    wide = starts(2 * size[1])
    narrow = starts(size[1])

    def step(row, slot):
        for col in wide:
            col = col + zero
            total = None
            for half in range(2):
                at_row, at_col = start[0] + 2 * row + half, start[1] + col
                value = right[at_row, pl.ds(at_col, 8), :] - applied(
                    source, fine, at_row, at_col, at_row - origin[0], at_col - origin[1]
                )
                total = value if total is None else total + value
            line[slot, pl.ds(col, 8), :] = total
        for col in narrow:
            value = line[slot, pl.ds(2 * col, 8, stride=2), :]
            value = value + line[slot, pl.ds(2 * col + 1, 8, stride=2), :]
            value = 0.25 * value
            if masked is not None:
                value = jnp.where(
                    coarse.inside(place[0] + row - masked[0], place[1] + col + zero - masked[1]),
                    value,
                    0.0,
                )
            out[place[0] + row, pl.ds(place[1] + col + zero, 8), :] = value

    by_rows(size[0], 2 * len(wide), step)


def prolong_into(out, place, add, source, start, size, line, zero):
    narrow = starts(size[1])
    wide = starts(2 * size[1])

    def step(row, slot):
        for col in narrow:
            value = source[start[0] + row, pl.ds(start[1] + col + zero, 8), :]
            line[slot, pl.ds(2 * col, 8, stride=2), :] = value
            line[slot, pl.ds(2 * col + 1, 8, stride=2), :] = value
        for col in wide:
            value = line[slot, pl.ds(col + zero, 8), :]
            for half in range(2):
                at_row, at_col = place[0] + 2 * row + half, place[1] + col + zero
                out[at_row, pl.ds(at_col, 8), :] = add[at_row, pl.ds(at_col, 8), :] + value

    by_rows(size[0], len(wide), step)


def clear(array):
    rows, cols = array.shape[0], array.shape[1]

    def step(row, slot):
        array[row] = jnp.zeros((cols, 128), jnp.float32)

    by_rows(rows, cols // 8, step)


def copy_block(out, out_at, source, source_at, size, zero):
    def body(row, col):
        out[out_at[0] + row, pl.ds(out_at[1] + col, 8), :] = source[
            source_at[0] + row, pl.ds(source_at[1] + col, 8), :
        ]

    each(size[0], size[1], zero, body)


def correlate(first, first_at, second, second_at, size, zero):
    cols = range(0, size[1], 8)
    count = rows_at_once(size[0], len(cols))

    def step(turn, sums):
        sums = list(sums)
        for row, col in [(turn * count + more, col) for more in range(count) for col in cols]:
            here = first[first_at[0] + row, pl.ds(first_at[1] + col + zero, 8), :]
            moved = (from_above(here), here, from_below(here))
            for a in range(3):
                for b in range(3):
                    window = second[
                        second_at[0] + row + a - 1, pl.ds(second_at[1] + col + zero + (b - 1), 8), :
                    ]
                    for c in range(3):
                        t = 9 * a + 3 * b + c
                        sums[t] = sums[t] + moved[c] * window
        return tuple(sums)

    blank = tuple(jnp.zeros((8, 128), jnp.float32) for _ in range(27))
    return lax.fori_loop(0, size[0] // count, step, blank)


def place_of(shape, mesh_shape, walls):
    gx, gy = lax.axis_index("gx"), second_index()
    levels = []
    for height in range(LOCAL):
        rows, cols = shape[0] >> height, shape[1] >> height
        levels.append(
            Level(walls, gx * rows, gy * cols, rows * mesh_shape[0], cols * mesh_shape[1])
        )
    return levels


def down_kernel(shape, mesh_shape, flip, *refs):
    (stencils, mask, still, low_first, block, high_first, low_second, high_second) = refs[:8]
    (kept, kept_pre, right1, pre1, right2) = refs[8:13]
    (wide, pre, line) = refs[13:]
    zero = still[0]
    walls = [mask[f].astype(jnp.float32) for f in range(6)]
    fine, middle = place_of(shape, mesh_shape, walls)
    rows, cols = shape[0], shape[1]
    copy_block(wide, (0, RIM0), low_first, (0, 0), (RIM0, cols), zero)
    copy_block(wide, (RIM0, RIM0), block, (0, 0), (rows, cols), zero)
    copy_block(wide, (RIM0 + rows, RIM0), high_first, (0, 0), (RIM0, cols), zero)
    copy_block(wide, (0, 0), low_second, (0, 0), (rows + 2 * RIM0, RIM0), zero)
    copy_block(wide, (0, RIM0 + cols), high_second, (0, 0), (rows + 2 * RIM0, RIM0), zero)
    before = LEVELS if flip else 0
    weights = weights_of(stencils, before, flip)
    origin = (RIM0, RIM0)
    smooth_into(
        pre, wide, weights, fine, (1, 1), (rows + 2 * RIM0 - 2, cols + 2 * RIM0 - 2), origin, zero
    )
    rows1, cols1 = rows // 2, cols // 2
    restrict_into(
        right1, (0, 0), wide, pre, line, fine, middle,
        (RIM0 - 2 * RIM1, RIM0 - 2 * RIM1), (rows1 + 2 * RIM1, cols1 + 2 * RIM1), origin, zero,
        (RIM1, RIM1),
    )
    inner = (RIM0 - KEEP, RIM0 - KEEP)
    size = (rows + 2 * KEEP, cols + 2 * KEEP)
    copy_block(kept, (0, 0), wide, inner, size, zero)
    copy_block(kept_pre, (0, 0), pre, inner, size, zero)
    weights = weights_of(stencils, before + 1, flip)
    clear(pre1)
    origin = (RIM1, RIM1)
    smooth_into(
        pre1, right1, weights, middle, (1, 1), (rows1 + 2 * RIM1 - 2, cols1 + 2 * RIM1 - 2),
        origin, zero,
    )
    restrict_into(
        right2, (0, 0), right1, pre1, line, middle, None, origin, (rows1 // 2, cols1 // 2), origin,
        zero, None,
    )


def up_kernel(shape, mesh_shape, flip, *refs):
    (stencils, mask, still), refs = refs[:3], refs[3:]
    cores = lax.axis_size("core")
    gathered, refs = refs[:cores], refs[cores:]
    (kept, kept_pre, right1, pre1), refs = refs[:4], refs[4:]
    if flip:
        (after0_fwd, kept_fwd, after1_fwd, right1_fwd), refs = refs[:4], refs[4:]
        slabs_fwd, refs = refs[:7], refs[7:]
        (answer, sums), refs = refs[:2], refs[2:]
        (after0, after1), refs = refs[:2], refs[2:]
    else:
        (target,), refs = refs[:1], refs[1:]
        (answer, error, after0, after1), refs = refs[:4], refs[4:]
        slabs_fwd = ()
        slabs, refs = refs[:7], refs[7:]
    (right2, mid2, after2, right3, mid3, after3, right4, mid4, rest1, rest2) = refs[:10]
    (mid1, result1, mid0, line) = refs[10:14]
    zero = still[0]
    walls = [mask[f].astype(jnp.float32) for f in range(6)]
    fine, middle = place_of(shape, mesh_shape, walls)
    gx, gy = lax.axis_index("gx"), second_index()
    across, along = mesh_shape
    rows2, cols2 = shape[0] // 4, shape[1] // 4
    before, later = (LEVELS, 0) if flip else (0, LEVELS)
    origin = (ROWS, COLS)
    for array in (right2, mid2, after2, right3, mid3, after3, right4, mid4, rest1, rest2):
        clear(array)

    def fill(peer, carry):
        for turn, source in enumerate(gathered):
            core = (lax.axis_index("core") + turn) % cores
            for other in range(along // cores):
                start = COLS + (other * cores + core) * cols2
                for row in range(rows2):
                    for col in range(0, cols2, 8):
                        right2[ROWS + peer * rows2 + row, pl.ds(start + col, 8), :] = source[
                            peer * (along // cores) + other, row, pl.ds(col, 8), :
                        ]
        return carry

    lax.fori_loop(0, across, fill, 0)
    grids = []
    for height in range(LOCAL, LEVELS + 1):
        total = ((shape[0] * across) >> height, (shape[1] * along) >> height)
        grids.append(Level(walls, 0, 0, *total))
    arrays = ((right2, mid2, after2), (right3, mid3, after3))
    coarser = (right3, right4)
    for step in range(2):
        right, mid, after = arrays[step]
        level = grids[step]
        weights = weights_of(stencils, before + LOCAL + step, flip)
        smooth_into(mid, right, weights, level, origin, level.total, origin, zero, masked=False)
        half = (level.total[0] // 2, level.total[1] // 2)
        restrict_into(
            coarser[step], origin, right, mid, line, level, None, origin, half, origin, zero, None
        )
    level = grids[2]
    weights = weights_of(stencils, 2 * LEVELS, flip)
    smooth_into(mid4, right4, weights, level, origin, level.total, origin, zero, masked=False)
    for rest in (rest1, rest2):
        remain_into(rest, right4, mid4, level, origin, level.total, origin, zero, masked=False)
        smooth_into(
            mid4, rest, weights, level, origin, level.total, origin, zero, masked=False, add=mid4
        )
    below = mid4
    for step in (1, 0):
        right, mid, after = arrays[step]
        level = grids[step]
        prolong_into(mid, origin, mid, below, origin, grids[step + 1].total, line, zero)
        remain_into(after, right, mid, level, origin, level.total, origin, zero, masked=False)
        weights = weights_of(stencils, later + LOCAL + step, flip)
        smooth_into(
            mid, after, weights, level, origin, level.total, origin, zero, masked=False, add=mid
        )
        below = mid
    rows1, cols1 = shape[0] // 2, shape[1] // 2
    half = RIM1 // 2
    prolong_into(
        mid1, (0, 0), pre1, below,
        (ROWS + gx * rows2 - half, COLS + gy * cols2 - half),
        (rows2 + 2 * half, cols2 + 2 * half), line, zero,
    )
    origin = (RIM1, RIM1)
    remain_into(
        after1, right1, mid1, middle, (2, 2), (rows1 + 2 * RIM1 - 4, cols1 + 2 * RIM1 - 4),
        origin, zero,
    )
    weights = weights_of(stencils, later + 1, flip)
    smooth_into(
        result1, after1, weights, middle, (3, 3), (rows1 + 2 * RIM1 - 6, cols1 + 2 * RIM1 - 6),
        origin, zero, add=mid1,
    )
    rows, cols = shape[0], shape[1]
    prolong_into(mid0, (0, 0), kept_pre, result1, (3, 3), (rows1 + 2, cols1 + 2), line, zero)
    origin = (KEEP, KEEP)
    remain_into(after0, kept, mid0, fine, (1, 1), (rows + 2, cols + 2), origin, zero)
    weights = weights_of(stencils, later, flip)

    def finish(row, col):
        value = smoothed(after0, weights, row + KEEP, col + KEEP)
        value = value + mid0[row + KEEP, pl.ds(col + KEEP, 8), :]
        answer[row, pl.ds(col, 8), :] = value
        if not flip:
            error[row, pl.ds(col, 8), :] = value - target[row, pl.ds(col, 8), :]

    each(rows, cols, zero, finish)
    kept_arrays = (
        (right2, grids[0]), (after2, grids[0]), (right3, grids[1]), (after3, grids[1]),
        (right4, grids[2]), (rest1, grids[2]), (rest2, grids[2]),
    )

    def own(level):
        return level.total[0] // across

    if not flip:
        for slab, (array, level) in zip(slabs, kept_arrays):
            count = own(level)
            for row in range(count + 2):
                slab[row] = array[ROWS - 1 + gx * count + row]
        return
    chosen = jnp.where(gy == 0, 1.0, 0.0)

    (part,) = refs[14:]

    def write(row, found, scale):
        for t in range(27):
            part[pl.ds(8 * (32 * row + t), 8), :] = scale * found[t]
        for t in range(27, 32):
            part[pl.ds(8 * (32 * row + t), 8), :] = jnp.zeros((8, 128), jnp.float32)

    mine = (KEEP, KEEP)
    write(LEVELS, correlate(kept, mine, after0_fwd, mine, (rows, cols), zero), 1.0)
    write(0, correlate(after0, mine, kept_fwd, mine, (rows, cols), zero), 1.0)
    mine = (RIM1, RIM1)
    write(LEVELS + 1, correlate(right1, mine, after1_fwd, mine, (rows1, cols1), zero), 4.0)
    write(1, correlate(after1, mine, right1_fwd, mine, (rows1, cols1), zero), 4.0)
    scale = 16.0
    for step in range(2):
        level = grids[step]
        right, mid, after = arrays[step]
        count = own(level)
        start = (ROWS + gx * count, COLS)
        size = (count, level.total[1])
        slab_right, slab_after = slabs_fwd[2 * step], slabs_fwd[2 * step + 1]
        found = correlate(right, start, slab_after, (1, COLS), size, zero)
        write(LEVELS + LOCAL + step, found, chosen * scale)
        found = correlate(after, start, slab_right, (1, COLS), size, zero)
        write(LOCAL + step, found, chosen * scale)
        scale *= 4.0
    level = grids[2]
    count = own(level)
    start = (ROWS + gx * count, COLS)
    size = (count, level.total[1])
    found = None
    for array, slab in ((right4, slabs_fwd[6]), (rest1, slabs_fwd[5]), (rest2, slabs_fwd[4])):
        more = correlate(array, start, slab, (1, COLS), size, zero)
        found = more if found is None else [x + y for x, y in zip(found, more)]
    write(2 * LEVELS, found, chosen * scale)
    ones = jnp.ones((8, 128), jnp.float32)
    folded = None
    for fold in range(8):
        more = part[pl.ds(fold, (2 * LEVELS + 1) * 32, stride=8), :]
        folded = more if folded is None else folded + more
    total = lax.dot_general(
        ones, folded, (((1,), (1,)), ((), ())),
        precision=lax.Precision.HIGHEST, preferred_element_type=jnp.float32,
    )
    sums[...] = total[0:1, :]


def final_kernel(scale, found, grads):
    total = jnp.sum(found[...].reshape(found.shape[0], found.shape[2]), axis=0, keepdims=True) * scale
    for row in range(grads.shape[0]):
        grads[row : row + 1, :] = total[0:1, 32 * row : 32 * row + grads.shape[1]]


def spaces(count_smem, arrays):
    smem = [pl.BlockSpec(memory_space=pltpu.SMEM)] * count_smem
    return smem + [pl.BlockSpec(memory_space=pltpu.VMEM)] * (len(arrays) - count_smem)


def padded(shape):
    whole = 4 * -(-shape[-1] // 128) * 128 * -(-shape[-2] // 8) * 8
    for size in shape[:-2]:
        whole *= size
    return whole


def near_enough(arrays):
    return max(padded(x.shape) for x in arrays) <= NEAR


def call(kernel, outs, scratch, arrays, name, far=(), smem=3):
    arrays = list(arrays)
    near = near_enough(arrays[smem:])
    if near:
        arrays[smem:] = [pltpu.with_memory_space_constraint(x, pltpu.VMEM) for x in arrays[smem:]]
    made = [
        pltpu.VMEM(shape, jnp.float32)
        if near and place not in far
        else jax.ShapeDtypeStruct(shape, jnp.float32)
        for place, shape in enumerate(outs)
    ]
    held = sum(padded(shape) for shape in list(outs) + list(scratch))
    held += sum(padded(x.shape) for x in arrays[smem:])
    return pl.pallas_call(
        kernel,
        out_shape=made,
        in_specs=spaces(smem, arrays),
        out_specs=[pl.BlockSpec(memory_space=pltpu.VMEM)] * len(outs),
        scratch_shapes=[pltpu.VMEM(shape, jnp.float32) for shape in scratch],
        compiler_params=pltpu.CompilerParams(vmem_limit_bytes=min(60 * 2**20, held + 4 * 2**20)),
        name=name,
    )(*arrays)


def shift_pair(low_part, high_part, axis):
    peers = lax.axis_size("gx") if axis == "gx" else second_size()
    even = (lax.axis_index("gx") if axis == "gx" else second_index()) % 2 == 0
    found = []
    for first, sent in ((0, jnp.where(even, high_part, low_part)), (1, jnp.where(even, low_part, high_part))):
        pairs = [(i, i + 1) for i in range(first, peers - 1, 2)]
        found.append(lax.ppermute(sent, axis, pairs + [(j, i) for i, j in pairs]))
    return jnp.where(even, found[1], found[0]), jnp.where(even, found[0], found[1])


def rim(block):
    rows, cols = block.shape[0], block.shape[1]
    low_first, high_first = shift_pair(block[:RIM0], block[rows - RIM0 :], "gx")
    tall_low = jnp.concatenate([low_first[:, :RIM0], block[:, :RIM0], high_first[:, :RIM0]], 0)
    tall_high = jnp.concatenate(
        [low_first[:, cols - RIM0 :], block[:, cols - RIM0 :], high_first[:, cols - RIM0 :]], 0
    )
    low_second, high_second = shift_pair(tall_low, tall_high, SECOND)
    return [low_first, block, high_first, low_second, high_second]


def share(block):
    peers = lax.axis_size("gx") * second_size()
    copies = jnp.broadcast_to(block[None], (peers,) + block.shape)
    return lax.all_to_all(copies, PEERS, 0, 0, tiled=True)


def share_by_pairs(block):
    peers = lax.axis_size("gx") * lax.axis_size("y")
    copies = jnp.broadcast_to(block[None], (peers,) + block.shape)
    mine = lax.all_to_all(copies, ("gx", "y"), 0, 0, tiled=True)
    if lax.axis_size("core") == 1:
        return [mine]
    return [mine, lax.ppermute(mine, "core", [(0, 1), (1, 0)])]


def on_device(rhs, target, stencils, face_mask):
    shape = rhs.shape
    mesh_shape = (lax.axis_size("gx"), second_size())
    rows, cols = shape[0], shape[1]
    still = jnp.zeros((1,), jnp.int32)
    small = [stencils, face_mask, still]
    wide = (rows + 2 * RIM0, cols + 2 * RIM0, 128)
    kept = (rows + 2 * KEEP, cols + 2 * KEEP, 128)
    wide1 = (rows // 2 + 2 * RIM1, cols // 2 + 2 * RIM1, 128)
    own2 = (rows // 4, cols // 4, 128)
    totals = [
        ((rows * mesh_shape[0]) >> h, (cols * mesh_shape[1]) >> h) for h in range(LOCAL, LEVELS + 1)
    ]
    whole = [(a + 2 * ROWS, b + 2 * COLS, 128) for a, b in totals]
    slab = [(a // mesh_shape[0] + 2, b + 2 * COLS, 128) for a, b in totals]
    slabs = [slab[0], slab[0], slab[1], slab[1], slab[2], slab[2], slab[2]]
    line = (SLOTS, -(-max(totals[0][1], wide[1]) // 8) * 8, 128)
    part = ((2 * LEVELS + 1) * 32 * 8, 128)
    scratch = [whole[0]] * 3 + [whole[1]] * 3 + [whole[2]] * 4 + [wide1, wide1, kept, line]

    def down(block, flip):
        return call(
            functools.partial(down_kernel, shape, mesh_shape, flip),
            [kept, kept, wide1, wide1, own2], [wide, wide, line], small + rim(block),
            "down_back" if flip else "down",
        )

    keep0, pre0, right1, pre1, right2 = down(rhs, False)
    answer, error, after0, after1, *kept_slabs = call(
        functools.partial(up_kernel, shape, mesh_shape, False),
        [shape, shape, kept, wide1] + slabs, scratch,
        small + share_by_pairs(right2) + [keep0, pre0, right1, pre1, target], "up", (0,),
    )
    back0, back_pre0, back1, back_pre1, back2 = down(error, True)
    grad_rhs, sums = call(
        functools.partial(up_kernel, shape, mesh_shape, True),
        [shape, (1, (2 * LEVELS + 1) * 32)], [kept, wide1] + scratch + [part],
        small + share_by_pairs(back2) + [back0, back_pre0, back1, back_pre1]
        + [after0, keep0, after1, right1] + list(kept_slabs), "up_back", (0,),
    )
    cells = rows * mesh_shape[0] * cols * mesh_shape[1] * shape[2]
    (grads,) = call(
        functools.partial(final_kernel, 1.0 / cells), [(2 * LEVELS + 1, 27)], [],
        [share(sums)], "final", (0,), 0,
    )
    return answer, grad_rhs, grads


def solution(mesh):
    along = mesh.shape["gy"]
    cores = 2 if along % 2 == 0 else 1
    parts = jax.sharding.Mesh(mesh.devices.reshape(-1, along // cores, cores), PEERS)
    block = P("gx", SECOND, None)
    return jax.shard_map(
        on_device,
        mesh=parts,
        in_specs=(block, block, P(), P()),
        out_specs=(block, block, P()),
        check_vma=False,
    )
```

```python
import functools

import jax
import jax.numpy as jnp
from jax import lax
from jax.experimental import pallas as pl
from jax.experimental.pallas import tpu as pltpu
from jax.sharding import PartitionSpec as P

LEVELS = 4
SWEEPS = 3
LOCAL = 2
RIM0 = 10
RIM1 = 4
KEEP = 2
ROWS, COLS = 2, 8
SECOND = ("y", "core")
PEERS = ("gx",) + SECOND
SLOTS = 4
BODY = 64
NEAR = 2**21


def second_index():
    return lax.axis_index("y") * lax.axis_size("core") + lax.axis_index("core")


def second_size():
    return lax.axis_size("y") * lax.axis_size("core")


def starts(width):
    places = list(range(0, width - 7, 8))
    if width % 8:
        places.append(width - 8)
    return places


def lanes(shape=(8, 128)):
    return lax.broadcasted_iota(jnp.int32, shape, 1)


def sublanes(shape=(8, 128)):
    return lax.broadcasted_iota(jnp.int32, shape, 0)


def from_below(value):
    return jnp.where(lanes(value.shape) == 0, 0.0, pltpu.roll(value, 1, 1))


def from_above(value):
    last = value.shape[1] - 1
    return jnp.where(lanes(value.shape) == last, 0.0, pltpu.roll(value, last, 1))


def weights_of(stencils, row, flip):
    return [stencils[row, 26 - t if flip else t] for t in range(27)]


class Level:
    def __init__(self, walls, first, second, total_first, total_second):
        self.walls = walls
        self.first = first
        self.second = second
        self.total = (total_first, total_second)

    def row_wall(self, row):
        at = self.first + row
        return jnp.where(at == 0, self.walls[0], 0.0) + jnp.where(
            at == self.total[0] - 1, self.walls[1], 0.0
        )

    def row_inside(self, row):
        at = self.first + row
        return (at >= 0) & (at < self.total[0])

    def wall_plane(self, col):
        at = self.second + col + sublanes()
        lane = lanes()
        plane = jnp.where(at == 0, self.walls[2], 0.0)
        plane = plane + jnp.where(at == self.total[1] - 1, self.walls[3], 0.0)
        plane = plane + jnp.where(lane == 0, self.walls[4], 0.0)
        return plane + jnp.where(lane == 127, self.walls[5], 0.0)

    def inside(self, row, col):
        at = self.second + col + sublanes()
        return self.row_inside(row) & (at >= 0) & (at < self.total[1])


def smoothed(source, weights, row, col):
    sums = [None, None, None]
    for a in range(3):
        for b in range(3):
            window = source[row + (a - 1), pl.ds(col + (b - 1), 8), :]
            for c in range(3):
                term = weights[9 * a + 3 * b + c] * window
                sums[c] = term if sums[c] is None else sums[c] + term
    return sums[1] + from_below(sums[0]) + from_above(sums[2])


def applied(source, level, row, col, at_row, at_col):
    here = source[row, pl.ds(col, 8), :]
    beside = source[row - 1, pl.ds(col, 8), :] + source[row + 1, pl.ds(col, 8), :]
    beside = beside + source[row, pl.ds(col - 1, 8), :] + source[row, pl.ds(col + 1, 8), :]
    beside = beside + from_below(here) + from_above(here)
    diagonal = (6.0 - level.row_wall(at_row)) - level.wall_plane(at_col)
    return diagonal * here - beside


def rows_at_once(rows, chunks):
    return max(n for n in range(1, rows + 1) if rows % n == 0 and (n == 1 or n * chunks <= BODY))


def by_rows(rows, chunks, step):
    count = rows_at_once(rows, chunks)

    def several(turn, carry):
        for row in range(count):
            step(turn * count + row, row % SLOTS)
        return carry

    lax.fori_loop(0, rows // count, several, 0)


def each(rows, cols, zero, body):
    places = starts(cols)

    def step(row, slot):
        for place in places:
            body(row, zero + place)

    by_rows(rows, len(places), step)


def smooth_into(out, source, weights, level, start, size, origin, zero, masked=True, add=None):
    def body(row, col):
        row, col = row + start[0], col + start[1]
        value = smoothed(source, weights, row, col)
        if masked:
            value = jnp.where(level.inside(row - origin[0], col - origin[1]), value, 0.0)
        if add is not None:
            value = value + add[row, pl.ds(col, 8), :]
        out[row, pl.ds(col, 8), :] = value

    each(size[0], size[1], zero, body)


def remain_into(out, right, source, level, start, size, origin, zero, masked=True):
    def body(row, col):
        row, col = row + start[0], col + start[1]
        value = right[row, pl.ds(col, 8), :] - applied(
            source, level, row, col, row - origin[0], col - origin[1]
        )
        if masked:
            value = jnp.where(level.inside(row - origin[0], col - origin[1]), value, 0.0)
        out[row, pl.ds(col, 8), :] = value

    each(size[0], size[1], zero, body)


def restrict_into(out, place, right, source, line, fine, coarse, start, size, origin, zero, masked):
    wide = starts(2 * size[1])
    narrow = starts(size[1])

    def step(row, slot):
        for col in wide:
            col = col + zero
            total = None
            for half in range(2):
                at_row, at_col = start[0] + 2 * row + half, start[1] + col
                value = right[at_row, pl.ds(at_col, 8), :] - applied(
                    source, fine, at_row, at_col, at_row - origin[0], at_col - origin[1]
                )
                total = value if total is None else total + value
            line[slot, pl.ds(col, 8), :] = total
        for col in narrow:
            value = line[slot, pl.ds(2 * col, 8, stride=2), :]
            value = value + line[slot, pl.ds(2 * col + 1, 8, stride=2), :]
            value = 0.25 * value
            if masked is not None:
                value = jnp.where(
                    coarse.inside(place[0] + row - masked[0], place[1] + col + zero - masked[1]),
                    value,
                    0.0,
                )
            out[place[0] + row, pl.ds(place[1] + col + zero, 8), :] = value

    by_rows(size[0], 2 * len(wide), step)


def prolong_into(out, place, add, source, start, size, line, zero):
    narrow = starts(size[1])
    wide = starts(2 * size[1])

    def step(row, slot):
        for col in narrow:
            value = source[start[0] + row, pl.ds(start[1] + col + zero, 8), :]
            line[slot, pl.ds(2 * col, 8, stride=2), :] = value
            line[slot, pl.ds(2 * col + 1, 8, stride=2), :] = value
        for col in wide:
            value = line[slot, pl.ds(col + zero, 8), :]
            for half in range(2):
                at_row, at_col = place[0] + 2 * row + half, place[1] + col + zero
                out[at_row, pl.ds(at_col, 8), :] = add[at_row, pl.ds(at_col, 8), :] + value

    by_rows(size[0], len(wide), step)


def clear(array):
    rows, cols = array.shape[0], array.shape[1]

    def step(row, slot):
        array[row] = jnp.zeros((cols, 128), jnp.float32)

    by_rows(rows, cols // 8, step)


def copy_block(out, out_at, source, source_at, size, zero):
    def body(row, col):
        out[out_at[0] + row, pl.ds(out_at[1] + col, 8), :] = source[
            source_at[0] + row, pl.ds(source_at[1] + col, 8), :
        ]

    each(size[0], size[1], zero, body)


def correlate(first, first_at, second, second_at, size, zero):
    cols = range(0, size[1], 8)
    count = rows_at_once(size[0], len(cols))

    def step(turn, sums):
        sums = list(sums)
        for row, col in [(turn * count + more, col) for more in range(count) for col in cols]:
            here = first[first_at[0] + row, pl.ds(first_at[1] + col + zero, 8), :]
            moved = (from_above(here), here, from_below(here))
            for a in range(3):
                for b in range(3):
                    window = second[
                        second_at[0] + row + a - 1, pl.ds(second_at[1] + col + zero + (b - 1), 8), :
                    ]
                    for c in range(3):
                        t = 9 * a + 3 * b + c
                        sums[t] = sums[t] + moved[c] * window
        return tuple(sums)

    blank = tuple(jnp.zeros((8, 128), jnp.float32) for _ in range(27))
    return lax.fori_loop(0, size[0] // count, step, blank)


def place_of(shape, mesh_shape, walls):
    gx, gy = lax.axis_index("gx"), second_index()
    levels = []
    for height in range(LOCAL):
        rows, cols = shape[0] >> height, shape[1] >> height
        levels.append(
            Level(walls, gx * rows, gy * cols, rows * mesh_shape[0], cols * mesh_shape[1])
        )
    return levels


def down_kernel(shape, mesh_shape, flip, *refs):
    (stencils, mask, still, low_first, block, high_first, low_second, high_second) = refs[:8]
    (kept, kept_pre, right1, pre1, right2) = refs[8:13]
    (wide, pre, line) = refs[13:]
    zero = still[0]
    walls = [mask[f].astype(jnp.float32) for f in range(6)]
    fine, middle = place_of(shape, mesh_shape, walls)
    rows, cols = shape[0], shape[1]
    copy_block(wide, (0, RIM0), low_first, (0, 0), (RIM0, cols), zero)
    copy_block(wide, (RIM0, RIM0), block, (0, 0), (rows, cols), zero)
    copy_block(wide, (RIM0 + rows, RIM0), high_first, (0, 0), (RIM0, cols), zero)

    def side(row, col):
        at = pl.ds(row * RIM0 + col, 8)
        wide[row, pl.ds(col, 8), :] = low_second[at, :]
        wide[row, pl.ds(RIM0 + cols + col, 8), :] = high_second[at, :]

    each(rows + 2 * RIM0, RIM0, zero, side)
    before = LEVELS if flip else 0
    weights = weights_of(stencils, before, flip)
    origin = (RIM0, RIM0)
    smooth_into(
        pre, wide, weights, fine, (1, 1), (rows + 2 * RIM0 - 2, cols + 2 * RIM0 - 2), origin, zero
    )
    rows1, cols1 = rows // 2, cols // 2
    restrict_into(
        right1, (0, 0), wide, pre, line, fine, middle,
        (RIM0 - 2 * RIM1, RIM0 - 2 * RIM1), (rows1 + 2 * RIM1, cols1 + 2 * RIM1), origin, zero,
        (RIM1, RIM1),
    )
    inner = (RIM0 - KEEP, RIM0 - KEEP)
    size = (rows + 2 * KEEP, cols + 2 * KEEP)
    copy_block(kept, (0, 0), wide, inner, size, zero)
    copy_block(kept_pre, (0, 0), pre, inner, size, zero)
    weights = weights_of(stencils, before + 1, flip)
    clear(pre1)
    origin = (RIM1, RIM1)
    smooth_into(
        pre1, right1, weights, middle, (1, 1), (rows1 + 2 * RIM1 - 2, cols1 + 2 * RIM1 - 2),
        origin, zero,
    )
    restrict_into(
        right2, (0, 0), right1, pre1, line, middle, None, origin, (rows1 // 2, cols1 // 2), origin,
        zero, None,
    )


def up_kernel(shape, mesh_shape, flip, *refs):
    (stencils, mask, still), refs = refs[:3], refs[3:]
    cores = lax.axis_size("core")
    gathered, refs = refs[:cores], refs[cores:]
    (kept, kept_pre, right1, pre1), refs = refs[:4], refs[4:]
    if flip:
        (after0_fwd, kept_fwd, after1_fwd, right1_fwd), refs = refs[:4], refs[4:]
        slabs_fwd, refs = refs[:7], refs[7:]
        (answer, sums), refs = refs[:2], refs[2:]
        (after0, after1), refs = refs[:2], refs[2:]
    else:
        (target,), refs = refs[:1], refs[1:]
        (answer, error, after0, after1), refs = refs[:4], refs[4:]
        slabs_fwd = ()
        slabs, refs = refs[:7], refs[7:]
    (right2, mid2, after2, right3, mid3, after3, right4, mid4, rest1, rest2) = refs[:10]
    (mid1, result1, mid0, line) = refs[10:14]
    zero = still[0]
    walls = [mask[f].astype(jnp.float32) for f in range(6)]
    fine, middle = place_of(shape, mesh_shape, walls)
    gx, gy = lax.axis_index("gx"), second_index()
    across, along = mesh_shape
    rows2, cols2 = shape[0] // 4, shape[1] // 4
    before, later = (LEVELS, 0) if flip else (0, LEVELS)
    origin = (ROWS, COLS)
    for array in (right2, mid2, after2, right3, mid3, after3, right4, mid4, rest1, rest2):
        clear(array)

    def fill(peer, carry):
        for turn, source in enumerate(gathered):
            core = (lax.axis_index("core") + turn) % cores
            for other in range(along // cores):
                start = COLS + (other * cores + core) * cols2
                for row in range(rows2):
                    for col in range(0, cols2, 8):
                        right2[ROWS + peer * rows2 + row, pl.ds(start + col, 8), :] = source[
                            peer * (along // cores) + other, row, pl.ds(col, 8), :
                        ]
        return carry

    lax.fori_loop(0, across, fill, 0)
    grids = []
    for height in range(LOCAL, LEVELS + 1):
        total = ((shape[0] * across) >> height, (shape[1] * along) >> height)
        grids.append(Level(walls, 0, 0, *total))
    arrays = ((right2, mid2, after2), (right3, mid3, after3))
    coarser = (right3, right4)
    for step in range(2):
        right, mid, after = arrays[step]
        level = grids[step]
        weights = weights_of(stencils, before + LOCAL + step, flip)
        smooth_into(mid, right, weights, level, origin, level.total, origin, zero, masked=False)
        half = (level.total[0] // 2, level.total[1] // 2)
        restrict_into(
            coarser[step], origin, right, mid, line, level, None, origin, half, origin, zero, None
        )
    level = grids[2]
    weights = weights_of(stencils, 2 * LEVELS, flip)
    smooth_into(mid4, right4, weights, level, origin, level.total, origin, zero, masked=False)
    for rest in (rest1, rest2):
        remain_into(rest, right4, mid4, level, origin, level.total, origin, zero, masked=False)
        smooth_into(
            mid4, rest, weights, level, origin, level.total, origin, zero, masked=False, add=mid4
        )
    below = mid4
    for step in (1, 0):
        right, mid, after = arrays[step]
        level = grids[step]
        prolong_into(mid, origin, mid, below, origin, grids[step + 1].total, line, zero)
        remain_into(after, right, mid, level, origin, level.total, origin, zero, masked=False)
        weights = weights_of(stencils, later + LOCAL + step, flip)
        smooth_into(
            mid, after, weights, level, origin, level.total, origin, zero, masked=False, add=mid
        )
        below = mid
    rows1, cols1 = shape[0] // 2, shape[1] // 2
    half = RIM1 // 2
    prolong_into(
        mid1, (0, 0), pre1, below,
        (ROWS + gx * rows2 - half, COLS + gy * cols2 - half),
        (rows2 + 2 * half, cols2 + 2 * half), line, zero,
    )
    origin = (RIM1, RIM1)
    remain_into(
        after1, right1, mid1, middle, (2, 2), (rows1 + 2 * RIM1 - 4, cols1 + 2 * RIM1 - 4),
        origin, zero,
    )
    weights = weights_of(stencils, later + 1, flip)
    smooth_into(
        result1, after1, weights, middle, (3, 3), (rows1 + 2 * RIM1 - 6, cols1 + 2 * RIM1 - 6),
        origin, zero, add=mid1,
    )
    rows, cols = shape[0], shape[1]
    prolong_into(mid0, (0, 0), kept_pre, result1, (3, 3), (rows1 + 2, cols1 + 2), line, zero)
    origin = (KEEP, KEEP)
    remain_into(after0, kept, mid0, fine, (1, 1), (rows + 2, cols + 2), origin, zero)
    weights = weights_of(stencils, later, flip)

    def finish(row, col):
        value = smoothed(after0, weights, row + KEEP, col + KEEP)
        value = value + mid0[row + KEEP, pl.ds(col + KEEP, 8), :]
        answer[row, pl.ds(col, 8), :] = value
        if not flip:
            error[row, pl.ds(col, 8), :] = value - target[row, pl.ds(col, 8), :]

    each(rows, cols, zero, finish)
    kept_arrays = (
        (right2, grids[0]), (after2, grids[0]), (right3, grids[1]), (after3, grids[1]),
        (right4, grids[2]), (rest1, grids[2]), (rest2, grids[2]),
    )

    def own(level):
        return level.total[0] // across

    if not flip:
        for slab, (array, level) in zip(slabs, kept_arrays):
            count = own(level)
            for row in range(count + 2):
                slab[row] = array[ROWS - 1 + gx * count + row]
        return
    chosen = jnp.where(gy == 0, 1.0, 0.0)

    (part,) = refs[14:]

    def write(row, found, scale):
        for t in range(27):
            part[pl.ds(8 * (32 * row + t), 8), :] = scale * found[t]
        for t in range(27, 32):
            part[pl.ds(8 * (32 * row + t), 8), :] = jnp.zeros((8, 128), jnp.float32)

    mine = (KEEP, KEEP)
    write(LEVELS, correlate(kept, mine, after0_fwd, mine, (rows, cols), zero), 1.0)
    write(0, correlate(after0, mine, kept_fwd, mine, (rows, cols), zero), 1.0)
    mine = (RIM1, RIM1)
    write(LEVELS + 1, correlate(right1, mine, after1_fwd, mine, (rows1, cols1), zero), 4.0)
    write(1, correlate(after1, mine, right1_fwd, mine, (rows1, cols1), zero), 4.0)
    scale = 16.0
    for step in range(2):
        level = grids[step]
        right, mid, after = arrays[step]
        count = own(level)
        start = (ROWS + gx * count, COLS)
        size = (count, level.total[1])
        slab_right, slab_after = slabs_fwd[2 * step], slabs_fwd[2 * step + 1]
        found = correlate(right, start, slab_after, (1, COLS), size, zero)
        write(LEVELS + LOCAL + step, found, chosen * scale)
        found = correlate(after, start, slab_right, (1, COLS), size, zero)
        write(LOCAL + step, found, chosen * scale)
        scale *= 4.0
    level = grids[2]
    count = own(level)
    start = (ROWS + gx * count, COLS)
    size = (count, level.total[1])
    found = None
    for array, slab in ((right4, slabs_fwd[6]), (rest1, slabs_fwd[5]), (rest2, slabs_fwd[4])):
        more = correlate(array, start, slab, (1, COLS), size, zero)
        found = more if found is None else [x + y for x, y in zip(found, more)]
    write(2 * LEVELS, found, chosen * scale)
    ones = jnp.ones((8, 128), jnp.float32)
    folded = None
    for fold in range(8):
        more = part[pl.ds(fold, (2 * LEVELS + 1) * 32, stride=8), :]
        folded = more if folded is None else folded + more
    total = lax.dot_general(
        ones, folded, (((1,), (1,)), ((), ())),
        precision=lax.Precision.HIGHEST, preferred_element_type=jnp.float32,
    )
    sums[...] = total[0:1, :]


def final_kernel(scale, found, grads):
    total = jnp.sum(found[...].reshape(found.shape[0], found.shape[2]), axis=0, keepdims=True) * scale
    for row in range(grads.shape[0]):
        grads[row : row + 1, :] = total[0:1, 32 * row : 32 * row + grads.shape[1]]


def spaces(count_smem, arrays):
    smem = [pl.BlockSpec(memory_space=pltpu.SMEM)] * count_smem
    return smem + [pl.BlockSpec(memory_space=pltpu.VMEM)] * (len(arrays) - count_smem)


def padded(shape):
    whole = 4 * -(-shape[-1] // 128) * 128 * -(-shape[-2] // 8) * 8
    for size in shape[:-2]:
        whole *= size
    return whole


def near_enough(arrays):
    return max(padded(x.shape) for x in arrays) <= NEAR


def call(kernel, outs, scratch, arrays, name, far=(), smem=3):
    arrays = list(arrays)
    near = near_enough(arrays[smem:])
    if near:
        arrays[smem:] = [pltpu.with_memory_space_constraint(x, pltpu.VMEM) for x in arrays[smem:]]
    made = [
        pltpu.VMEM(shape, jnp.float32)
        if near and place not in far
        else jax.ShapeDtypeStruct(shape, jnp.float32)
        for place, shape in enumerate(outs)
    ]
    held = sum(padded(shape) for shape in list(outs) + list(scratch))
    held += sum(padded(x.shape) for x in arrays[smem:])
    return pl.pallas_call(
        kernel,
        out_shape=made,
        in_specs=spaces(smem, arrays),
        out_specs=[pl.BlockSpec(memory_space=pltpu.VMEM)] * len(outs),
        scratch_shapes=[pltpu.VMEM(shape, jnp.float32) for shape in scratch],
        compiler_params=pltpu.CompilerParams(vmem_limit_bytes=min(60 * 2**20, held + 4 * 2**20)),
        name=name,
    )(*arrays)


def shift_pair(low_part, high_part, axis):
    peers = lax.axis_size("gx") if axis == "gx" else second_size()
    even = (lax.axis_index("gx") if axis == "gx" else second_index()) % 2 == 0
    found = []
    for first, sent in ((0, jnp.where(even, high_part, low_part)), (1, jnp.where(even, low_part, high_part))):
        pairs = [(i, i + 1) for i in range(first, peers - 1, 2)]
        found.append(lax.ppermute(sent, axis, pairs + [(j, i) for i, j in pairs]))
    return jnp.where(even, found[1], found[0]), jnp.where(even, found[0], found[1])


def rim(block):
    rows, cols = block.shape[0], block.shape[1]
    low_first, high_first = shift_pair(block[:RIM0], block[rows - RIM0 :], "gx")
    tall_low = jnp.concatenate([low_first[:, :RIM0], block[:, :RIM0], high_first[:, :RIM0]], 0)
    tall_high = jnp.concatenate(
        [low_first[:, cols - RIM0 :], block[:, cols - RIM0 :], high_first[:, cols - RIM0 :]], 0
    )
    low_second, high_second = shift_pair(
        tall_low.reshape(-1, block.shape[2]), tall_high.reshape(-1, block.shape[2]), SECOND
    )
    return [low_first, block, high_first, low_second, high_second]


def share(block):
    peers = lax.axis_size("gx") * second_size()
    copies = jnp.broadcast_to(block[None], (peers,) + block.shape)
    return lax.all_to_all(copies, PEERS, 0, 0, tiled=True)


def share_by_pairs(block):
    peers = lax.axis_size("gx") * lax.axis_size("y")
    copies = jnp.broadcast_to(block[None], (peers,) + block.shape)
    mine = lax.all_to_all(copies, ("gx", "y"), 0, 0, tiled=True)
    if lax.axis_size("core") == 1:
        return [mine]
    return [mine, lax.ppermute(mine, "core", [(0, 1), (1, 0)])]


def on_device(rhs, target, stencils, face_mask):
    shape = rhs.shape
    mesh_shape = (lax.axis_size("gx"), second_size())
    rows, cols = shape[0], shape[1]
    still = jnp.zeros((1,), jnp.int32)
    small = [stencils, face_mask, still]
    wide = (rows + 2 * RIM0, cols + 2 * RIM0, 128)
    kept = (rows + 2 * KEEP, cols + 2 * KEEP, 128)
    wide1 = (rows // 2 + 2 * RIM1, cols // 2 + 2 * RIM1, 128)
    own2 = (rows // 4, cols // 4, 128)
    totals = [
        ((rows * mesh_shape[0]) >> h, (cols * mesh_shape[1]) >> h) for h in range(LOCAL, LEVELS + 1)
    ]
    whole = [(a + 2 * ROWS, b + 2 * COLS, 128) for a, b in totals]
    slab = [(a // mesh_shape[0] + 2, b + 2 * COLS, 128) for a, b in totals]
    slabs = [slab[0], slab[0], slab[1], slab[1], slab[2], slab[2], slab[2]]
    line = (SLOTS, -(-max(totals[0][1], wide[1]) // 8) * 8, 128)
    part = ((2 * LEVELS + 1) * 32 * 8, 128)
    scratch = [whole[0]] * 3 + [whole[1]] * 3 + [whole[2]] * 4 + [wide1, wide1, kept, line]

    def down(block, flip):
        return call(
            functools.partial(down_kernel, shape, mesh_shape, flip),
            [kept, kept, wide1, wide1, own2], [wide, wide, line], small + rim(block),
            "down_back" if flip else "down",
        )

    keep0, pre0, right1, pre1, right2 = down(rhs, False)
    answer, error, after0, after1, *kept_slabs = call(
        functools.partial(up_kernel, shape, mesh_shape, False),
        [shape, shape, kept, wide1] + slabs, scratch,
        small + share_by_pairs(right2) + [keep0, pre0, right1, pre1, target], "up", (0,),
    )
    back0, back_pre0, back1, back_pre1, back2 = down(error, True)
    grad_rhs, sums = call(
        functools.partial(up_kernel, shape, mesh_shape, True),
        [shape, (1, (2 * LEVELS + 1) * 32)], [kept, wide1] + scratch + [part],
        small + share_by_pairs(back2) + [back0, back_pre0, back1, back_pre1]
        + [after0, keep0, after1, right1] + list(kept_slabs), "up_back", (0,),
    )
    cells = rows * mesh_shape[0] * cols * mesh_shape[1] * shape[2]
    (grads,) = call(
        functools.partial(final_kernel, 1.0 / cells), [(2 * LEVELS + 1, 27)], [],
        [share(sums)], "final", (0,), 0,
    )
    return answer, grad_rhs, grads


def solution(mesh):
    along = mesh.shape["gy"]
    cores = 2 if along % 2 == 0 else 1
    parts = jax.sharding.Mesh(mesh.devices.reshape(-1, along // cores, cores), PEERS)
    block = P("gx", SECOND, None)
    return jax.shard_map(
        on_device,
        mesh=parts,
        in_specs=(block, block, P(), P()),
        out_specs=(block, block, P()),
        check_vma=False,
    )
```
